32 devices in a mesh: blk: 8 (over y, x, core), ulysses: 4 (over z).
Axes of the slice: x: 2, y: 2, z: 4, core: 2. Of those that a mesh axis runs over, the one named last changes fastest.
Arguments:
- tokens: bfloat16 [2048, 3072], P(('blk', 'ulysses')), may hold values from -6 to 6
- mod_shift: float32 [3072], replicated, may hold values from -3 to 3
- mod_scale: float32 [3072], replicated, may hold values from -3 to 3
- mod_gate: float32 [3072], replicated, may hold values from 0.5 to 1.5
- qkv_weight: bfloat16 [3, 3072, 3072], P(None, None, 'ulysses'), may hold values from -0.109375 to 0.109375
- query_gain: float32 [128], replicated, may hold values from 1 to 16
- key_gain: float32 [128], replicated, may hold values from 1 to 16
- out_weight: bfloat16 [3072, 3072], P(None, 'ulysses'), may hold values from -0.109375 to 0.109375
Outputs:
- mixed: bfloat16 [2048, 3072], P(('blk', 'ulysses'))
The draws below stay inside these ranges and needn't reach their ends.
All inputs are finite; a program needn't handle non-finite values.
Results may differ from the reference program's by a relative error of at most 0.013.
The reference program's roundings to bfloat16 on the way (of `modulated`, `queries`, `keys`, `values`, `powers` and `attended`) count: a program that leaves them out, or rounds other values in their place, can miss the bound.
Values may be sent and summed in bfloat16 or wider, within the bound.
A program may use at most 128 MiB of HBM per device.

```python
import math
import jax
import jax.numpy as jnp
from jax import lax

D = 3072
HEADS = 24
HEAD_DIM = 128
SEQ = 2048


def gain_vector(key, salt):
    base = jnp.exp(jax.random.uniform(jax.random.fold_in(key, salt), (HEAD_DIM,), jnp.float32, 0.0, 1.1))
    return base


def draw_query_gain(key, part):
    return gain_vector(key, 1)


def draw_key_gain(key, part):
    return gain_vector(key, 2)


def block_levels(stream_key, shape, shards, smallest, high):
    factor_of = 1.0
    for dim, blocks in shards:
        heights = jax.random.uniform(jax.random.fold_in(jax.random.fold_in(stream_key, 6), dim), (blocks,), jnp.float32, smallest / len(shards), high / len(shards))
        factor_of = factor_of * jnp.repeat(jnp.exp(heights), shape[dim] // blocks).reshape((-1,) + (1,) * (len(shape) - 1 - dim))
    return factor_of


def bell_draw(stream_key, shape, width, bound, cuts=(), held_as=jnp.bfloat16):
    loudness = block_levels(stream_key, shape, cuts, -0.22, 0.18) if cuts else 1.0
    values = jax.random.normal(stream_key, shape, jnp.float32) * width * loudness
    return jnp.minimum(jnp.maximum(values, -bound), bound).astype(held_as)


def setup_inputs(seed: int = 0) -> dict:
    streams_of = jax.random.split(jax.random.key(seed), 9)
    return {
        "tokens": bell_draw(streams_of[0], (SEQ, D), 1.0, 6.0, ((0, 32),)),
        "mod_shift": bell_draw(streams_of[1], (D,), 0.5, 3.0, (), jnp.float32),
        "mod_scale": bell_draw(streams_of[2], (D,), 0.5, 3.0, (), jnp.float32),
        "mod_gate": jnp.clip(jax.random.uniform(streams_of[3], (D,), jnp.float32, 0.5, 1.5), 0.5, 1.5),
        "qkv_weight": bell_draw(streams_of[4], (3, D, HEADS * HEAD_DIM), D ** -0.5, 0.109375, ((2, 4),)),
        "query_gain": draw_query_gain(jax.random.fold_in(streams_of[8], 71), 0),
        "key_gain": draw_key_gain(jax.random.fold_in(streams_of[8], 71), 0),
        "out_weight": bell_draw(streams_of[7], (HEADS * HEAD_DIM, D), (HEADS * HEAD_DIM) ** -0.5, 0.109375, ((1, 4),)),
    }


def head_norm(projected, gain, factor):
    split = projected.reshape(projected.shape[0], -1, gain.shape[0])
    meansq = lax.optimization_barrier(jnp.mean(split * split, axis=-1, keepdims=True))
    return (split * lax.rsqrt(meansq + 1e-06) * gain * factor).reshape(projected.shape)

def reference(tokens, mod_shift, mod_scale, mod_gate, qkv_weight, query_gain, key_gain, out_weight):
    wide = tokens.astype(jnp.float32)
    center = lax.optimization_barrier(jnp.mean(wide, axis=-1, keepdims=True))
    spread = lax.optimization_barrier(jnp.mean((wide - center) ** 2, axis=-1, keepdims=True))
    normed = (wide - center) / jnp.sqrt(spread + 1e-06)
    modulated = (normed * (1.0 + mod_scale) + mod_shift).astype(jnp.bfloat16)
    query_sums = jnp.dot(modulated, qkv_weight[0], preferred_element_type=jnp.float32)
    key_sums = jnp.dot(modulated, qkv_weight[1], preferred_element_type=jnp.float32)
    value_sums = jnp.dot(modulated, qkv_weight[2], preferred_element_type=jnp.float32)
    queries = head_norm(query_sums, query_gain, 1.0 / math.sqrt(HEAD_DIM)).astype(jnp.bfloat16)
    keys = head_norm(key_sums, key_gain, 1.0).astype(jnp.bfloat16)
    values = value_sums.astype(jnp.bfloat16)
    length = tokens.shape[0]
    block = math.gcd(length, 1024)

    def heads_first(matrix):
        return matrix.reshape(length, HEADS, HEAD_DIM).transpose(1, 0, 2)

    def one_head(operands):
        query_head, key_head, value_head = operands

        def one_block(query_block):
            scores = jnp.dot(query_block, key_head.T, preferred_element_type=jnp.float32)
            highest = lax.optimization_barrier(jnp.max(scores, axis=-1, keepdims=True))
            powers = jnp.exp(scores - highest)
            numerator = jnp.dot(powers.astype(jnp.bfloat16), value_head, preferred_element_type=jnp.float32)
            return numerator / lax.optimization_barrier(jnp.sum(powers, axis=-1, keepdims=True))
        result = lax.map(one_block, query_head.reshape(length // block, block, HEAD_DIM))
        return result.reshape(length, HEAD_DIM)
    attended = lax.map(one_head, (heads_first(queries), heads_first(keys), heads_first(values)))
    attended = attended.transpose(1, 0, 2).reshape(length, HEADS * HEAD_DIM).astype(jnp.bfloat16)
    branch = jnp.dot(attended, out_weight, preferred_element_type=jnp.float32)
    return (wide + mod_gate * branch).astype(jnp.bfloat16)
```

```python
import functools
import math

import jax
import jax.numpy as jnp
from jax import lax
from jax.experimental import pallas as pl
from jax.experimental.pallas import tpu as pltpu
from jax.sharding import PartitionSpec as P

MESH = pl.DeviceIdType.MESH
BF = jnp.bfloat16
F32 = jnp.float32
SPLIT = 2


def highest_bit(mask):
    return 1 << (mask.bit_length() - 1)


def lowest_bit(mask):
    return mask & -mask


def source_slot(mask, part):
    if mask & 1:
        return mask - 1, 1
    bit = highest_bit(mask) if part == 0 else lowest_bit(mask)
    return mask - bit, bit


def kernel(
    n_u, n_blk,
    tok_ref, shift_ref, scale_ref, gate_ref, w_hbm, qg_ref, kg_ref, wo_hbm, out_ref,
    w_ref, wo_ref, mod, q_ref, kv, att, stage, br,
    w_sem, sa_r, sa_l, ra, sb, rb, sc_r, sc_l, rc, sd, rd,
):
    z = lax.axis_index("ulysses")
    b = lax.axis_index("blk")
    rows, model = tok_ref.shape
    head = qg_ref.shape[1]
    width = w_ref.shape[2]
    heads = width // head
    factor = 1.0 / math.sqrt(head)
    last = n_u - 1
    half = rows // 2
    bits = [1 << i for i in range(n_blk.bit_length() - 1)]
    pair = 2 if heads % 2 == 0 else heads
    tile = pair * head

    for j in (1, 2, 0):
        pltpu.make_async_copy(w_hbm.at[j], w_ref.at[j], w_sem.at[j]).start()
    pltpu.make_async_copy(wo_hbm, wo_ref, w_sem.at[3]).start()

    def flip(bit):
        return b + (1 - 2 * ((b // bit) % 2)) * bit

    barrier = pltpu.get_barrier_semaphore()
    for d in range(1, n_u):
        pl.semaphore_signal(
            barrier, inc=1, device_id={"ulysses": (z + d) % n_u}, device_id_type=MESH
        )
    for bit in bits:
        pl.semaphore_signal(barrier, inc=1, device_id={"blk": flip(bit)}, device_id_type=MESH)

    wide = tok_ref[...].astype(F32)
    center = jnp.mean(wide, axis=-1, keepdims=True)
    spread = jnp.mean((wide - center) ** 2, axis=-1, keepdims=True)
    normed = (wide - center) * lax.rsqrt(spread + 1e-06)
    modulated = (normed * (1.0 + scale_ref[...]) + shift_ref[...]).astype(BF)
    mod[pl.ds(2 * z, 2)] = modulated.reshape(2, half, model)

    pl.semaphore_wait(barrier, n_u - 1 + len(bits))

    def line_copy(buf, index, send, recv, step):
        return pltpu.make_async_remote_copy(
            src_ref=buf.at[index], dst_ref=buf.at[index],
            send_sem=send.at[index], recv_sem=recv.at[index],
            device_id={"ulysses": z + step}, device_id_type=MESH,
        )

    def a_right(o):
        return line_copy(mod, o, sa_r, ra, 1)

    def a_left(o):
        return line_copy(mod, o, sa_l, ra, -1)

    def b_copy(mask, part, s):
        slot, bit = source_slot(mask, part)
        return pltpu.make_async_remote_copy(
            src_ref=kv.at[part, :, slot, s], dst_ref=kv.at[part, :, mask, s],
            send_sem=sb.at[mask, part, s], recv_sem=rb.at[mask, part, s],
            device_id={"blk": flip(bit)}, device_id_type=MESH,
        )

    masks = range(1, n_blk)

    def b_send(slot, part, s):
        for mask in sorted(masks, key=lambda m: m & 1):
            if source_slot(mask, part)[0] == slot:
                b_copy(mask, part, s).start()

    def b_level(level, s):
        for part in (0, 1):
            for mask in masks:
                if mask % 2 == 0 and bin(mask).count("1") == level:
                    b_copy(mask, part, s).wait_recv()
                    b_send(mask, part, s)

    levels = range(1, len(bits))

    def head_norm(sums, gain, scale):
        meansq = jnp.mean(sums * sums, axis=-1, keepdims=True)
        return sums * lax.rsqrt(meansq + 1e-06) * gain * scale

    def project(j, first, count, put):
        def body(i, _):
            start = pl.multiple_of(i * tile, tile)
            sums = jnp.dot(
                mod[pl.ds(first, count)].reshape(count * half, model),
                w_ref[j, :, pl.ds(start, tile)],
                preferred_element_type=F32,
            )
            for e in range(pair):
                put(i * pair + e, sums[:, e * head:(e + 1) * head])
            return 0

        lax.fori_loop(0, heads // pair, body, 0)

    def project_chunk(first, count, own=False):
        units = pl.ds(first, count)

        def ready(j):
            if own:
                pltpu.make_async_copy(w_hbm.at[j], w_ref.at[j], w_sem.at[j]).wait()

        def put_key(h, sums):
            keys = head_norm(sums, kg_ref[...], 1.0).astype(BF)
            kv[0, h, 0, units] = keys.reshape(count, half, head)

        def put_value(h, sums):
            kv[1, h, 0, units] = sums.astype(BF).reshape(count, half, head)

        def put_query(h, sums):
            queries = head_norm(sums, qg_ref[...], factor).astype(BF)
            q_ref[h, units] = queries.reshape(count, half, head)

        ready(1)
        project(1, first, count, put_key)
        for u in range(count):
            b_send(0, 0, first + u)
        ready(2)
        project(2, first, count, put_value)
        for u in range(count):
            b_send(0, 1, first + u)
        ready(0)
        project(0, first, count, put_query)

    for u in range(2):
        @pl.when(z < last)
        def _():
            a_right(2 * z + u).start()

        @pl.when(z > 0)
        def _():
            a_left(2 * z + u).start()

    project_chunk(2 * z, 2, own=True)

    def at_distance(k, act):
        for side in (-1, 1):
            o = z + side * k

            @pl.when((o >= 0) & (o <= last))
            def _():
                act(o)

    def pass_levels(which):
        def act(o):
            for level in which:
                for u in range(2):
                    b_level(level, 2 * o + u)
        return act

    def receive(k):
        for u in range(2):
            @pl.when(z - k >= 0)
            def _():
                a_right(2 * (z - k) + u).wait_recv()

                @pl.when(z < last)
                def _():
                    a_right(2 * (z - k) + u).start()

            @pl.when(z + k <= last)
            def _():
                a_left(2 * (z + k) + u).wait_recv()

                @pl.when(z > 0)
                def _():
                    a_left(2 * (z + k) + u).start()

    def previous(k, which):
        if isinstance(k, int) and k == 1:
            pass_levels(which)(z)
        else:
            at_distance(k - 1, pass_levels(which))

    for k in range(1, last):
        receive(k)
        previous(k, levels[:1])
        at_distance(k, lambda o: project_chunk(2 * o, 2))
        previous(k, levels[1:])

    ends = (z == 0) | (z == last)
    far = last - z

    def far_half(u):
        @pl.when(ends)
        def _():
            @pl.when(z == 0)
            def _():
                a_left(2 * far + u).wait_recv()

            @pl.when(z > 0)
            def _():
                a_right(2 * far + u).wait_recv()

            project_chunk(2 * far + u, 1)

    def far_levels(u, which):
        @pl.when(ends)
        def _():
            for level in which:
                b_level(level, 2 * far + u)

    previous(last, levels[:1])
    far_half(0)
    previous(last, levels[1:])
    far_levels(0, levels[:1])
    far_half(1)
    far_levels(0, levels[1:])
    far_levels(1, levels)

    def b_finish(s, _):
        for part in (0, 1):
            for mask in masks:
                if mask % 2 == 1:
                    b_copy(mask, part, s).wait_recv()
        return 0

    lax.fori_loop(0, 2 * n_u, b_finish, 0)
    pltpu.make_async_copy(wo_hbm, wo_ref, w_sem.at[3]).wait()

    keys_all = n_blk * n_u * rows

    def order(i):
        return jnp.where(i % 2 == 0, i // 2, last - i // 2)

    def c_right(o, src):
        return pltpu.make_async_remote_copy(
            src_ref=att.at[o, src], dst_ref=att.at[o, src],
            send_sem=sc_r.at[o, src], recv_sem=rc.at[o, src],
            device_id={"ulysses": z + 1}, device_id_type=MESH,
        )

    def c_left(o, src):
        return pltpu.make_async_remote_copy(
            src_ref=att.at[o, src], dst_ref=att.at[o, src],
            send_sem=sc_l.at[o, src], recv_sem=rc.at[o, src],
            device_id={"ulysses": z - 1}, device_id_type=MESH,
        )

    def d_copy(o, src):
        return pltpu.make_async_remote_copy(
            src_ref=stage.at[o], dst_ref=br.at[src],
            send_sem=sd.at[o], recv_sem=rd.at[src],
            device_id={"ulysses": o}, device_id_type=MESH,
        )

    group = 2 if n_u % 2 == 0 else 1

    def attend(chunks):
        for h in range(heads):
            keys = kv[0, h].reshape(keys_all, head)
            values = kv[1, h].reshape(keys_all, head)
            queries = jnp.concatenate(
                [q_ref[h, pl.ds(2 * o, 2)].reshape(rows, head) for o in chunks], axis=0
            )
            scores = lax.dot_general(
                queries, keys, (((1,), (1,)), ((), ())), preferred_element_type=F32
            )
            powers = jnp.exp(scores - jnp.max(scores, axis=-1, keepdims=True))
            total = jnp.sum(powers, axis=-1, keepdims=True)
            numerator = jnp.dot(powers.astype(BF), values, preferred_element_type=F32)
            result = (numerator / total).astype(BF)
            for g, o in enumerate(chunks):
                att[o, z, :, h * head:(h + 1) * head] = result[g * rows:(g + 1) * rows]

    def pass_right(o, src):
        c_right(o, src).wait_recv()

        @pl.when(z < last)
        def _():
            c_right(o, src).start()

    def pass_left(o, src):
        c_left(o, src).wait_recv()

        @pl.when(z > 0)
        def _():
            c_left(o, src).start()

    low = z < n_u // 2

    def attend_step(t, _):
        @pl.when(t < n_u // group)
        def _():
            chunks = [order(group * t + g) for g in range(group)]
            attend(chunks)
            for o in chunks:
                @pl.when(z < last)
                def _():
                    c_right(o, z).start()

                @pl.when(z > 0)
                def _():
                    c_left(o, z).start()

        for g in range(group):
            @pl.when((t > 0) & low & (z > 0))
            def _():
                pass_left(order(group * (t - 1) + g), z + 1)

            @pl.when((t > 0) & jnp.logical_not(low) & (z < last))
            def _():
                pass_right(order(group * (t - 1) + g), z - 1)

        return 0

    lax.fori_loop(0, n_u // group + 1, attend_step, 0)

    def mix_step(t, _):
        for k in range(last, 0, -1):
            i = t - k + 1
            held = (i >= 0) & (i < n_u)
            right_too = held & (z - k >= 0)
            left_too = held & (z + k <= last)
            if k == 1:
                right_too = right_too & (low | (z == last))
                left_too = left_too & (jnp.logical_not(low) | (z == 0))

            @pl.when(right_too)
            def _():
                pass_right(order(i), z - k)

            @pl.when(left_too)
            def _():
                pass_left(order(i), z + k)

        @pl.when(t >= last - 1)
        def _():
            o = order(t - last + 1)
            total = jnp.zeros((rows, width), F32)
            for src in range(n_u):
                total += jnp.dot(
                    att[o, src], wo_ref[src * width:(src + 1) * width, :],
                    preferred_element_type=F32,
                )

            @pl.when(o == z)
            def _():
                br[z] = total.astype(BF)

            @pl.when(o != z)
            def _():
                stage[o] = total.astype(BF)
                d_copy(o, z).start()

        return 0

    lax.fori_loop(0, n_u + last - 1, mix_step, 0)

    for src in range(n_u):
        @pl.when(src != z)
        def _():
            d_copy(src, src).wait_recv()

        cols = slice(src * width, (src + 1) * width)
        out_ref[:, cols] = (
            tok_ref[:, cols].astype(F32) + gate_ref[:, cols] * br[src].astype(F32)
        ).astype(BF)

    def finish(s, _):
        for u in range(2):
            @pl.when((s <= z) & (z < last))
            def _():
                a_right(2 * s + u).wait_send()

            @pl.when((s >= z) & (z > 0))
            def _():
                a_left(2 * s + u).wait_send()

        for src in range(n_u):
            @pl.when((src <= z) & (z < last))
            def _():
                c_right(s, src).wait_send()

            @pl.when((src >= z) & (z > 0))
            def _():
                c_left(s, src).wait_send()

        @pl.when(s != z)
        def _():
            d_copy(s, z).wait_send()

        for part in (0, 1):
            for mask in masks:
                for u in range(2):
                    b_copy(mask, part, 2 * s + u).wait_send()
        return 0

    lax.fori_loop(0, n_u, finish, 0)


def split_kernel(
    n_u, n_blk,
    tok_ref, shift_ref, scale_ref, gate_ref, w_hbm, qg_ref, kg_ref, wo_hbm, out_ref,
    w_ref, wo_ref, mod, q_ref, kv, att, xatt, stage, br,
    w_sem, sa_r, sa_l, ra, sb, rb, sq, rq, sx, rx, sc_r, sc_l, rc, sd, rd,
):
    z = lax.axis_index("ulysses")
    b = lax.axis_index("blk")
    rows, model = tok_ref.shape
    head = qg_ref.shape[1]
    width = w_ref.shape[2]
    heads = width // head
    share = heads // 2
    cols = share * head
    factor = 1.0 / math.sqrt(head)
    last = n_u - 1
    half = rows // 2
    bits = [1 << i for i in range(n_blk.bit_length() - 1)]
    masks = range(1, n_blk)
    side = (b // SPLIT) % 2
    mine = side * share
    theirs = (1 - side) * share

    for j in (1, 2, 0):
        pltpu.make_async_copy(w_hbm.at[j], w_ref.at[j], w_sem.at[j]).start()
    pltpu.make_async_copy(wo_hbm, wo_ref, w_sem.at[3]).start()

    def flip(bit):
        return b + (1 - 2 * ((b // bit) % 2)) * bit

    barrier = pltpu.get_barrier_semaphore()
    for d in range(1, n_u):
        pl.semaphore_signal(
            barrier, inc=1, device_id={"ulysses": (z + d) % n_u}, device_id_type=MESH
        )
    for bit in bits:
        pl.semaphore_signal(barrier, inc=1, device_id={"blk": flip(bit)}, device_id_type=MESH)

    wide = tok_ref[...].astype(F32)
    center = jnp.mean(wide, axis=-1, keepdims=True)
    spread = jnp.mean((wide - center) ** 2, axis=-1, keepdims=True)
    normed = (wide - center) * lax.rsqrt(spread + 1e-06)
    modulated = (normed * (1.0 + scale_ref[...]) + shift_ref[...]).astype(BF)
    mod[pl.ds(2 * z, 2)] = modulated.reshape(2, half, model)

    with jax.named_scope("barrier"):
        pl.semaphore_wait(barrier, n_u - 1 + len(bits))

    def line_copy(buf, index, send, recv, step):
        return pltpu.make_async_remote_copy(
            src_ref=buf.at[index], dst_ref=buf.at[index],
            send_sem=send.at[index], recv_sem=recv.at[index],
            device_id={"ulysses": z + step}, device_id_type=MESH,
        )

    def a_right(o):
        return line_copy(mod, o, sa_r, ra, 1)

    def a_left(o):
        return line_copy(mod, o, sa_l, ra, -1)

    def source(mask, part):
        if mask & 1:
            return mask - 1, 1
        if mask == SPLIT:
            return 0, SPLIT
        rest = mask & ~SPLIT
        bit = highest_bit(rest) if part == 0 else lowest_bit(rest)
        return mask - bit, bit

    def b_copy(mask, part, u):
        slot, bit = source(mask, part)
        own = pl.ds(theirs if bit == SPLIT else mine, share)
        return pltpu.make_async_remote_copy(
            src_ref=kv.at[part, own, slot, u], dst_ref=kv.at[part, own, mask, u],
            send_sem=sb.at[mask, part, u], recv_sem=rb.at[mask, part, u],
            device_id={"blk": flip(bit)}, device_id_type=MESH,
        )

    def b_wait(mask, part, u):
        here = kv.at[part, pl.ds(mine, share), mask, u]
        pltpu.make_async_remote_copy(
            src_ref=here, dst_ref=here,
            send_sem=sb.at[mask, part, u], recv_sem=rb.at[mask, part, u],
            device_id={"blk": flip(source(mask, part)[1])}, device_id_type=MESH,
        ).wait_recv()

    def q_copy(u, first):
        heads_of = pl.ds(first, share)
        return pltpu.make_async_remote_copy(
            src_ref=q_ref.at[heads_of, 0, u], dst_ref=q_ref.at[heads_of, 1, u],
            send_sem=sq.at[u], recv_sem=rq.at[u],
            device_id={"blk": flip(SPLIT)}, device_id_type=MESH,
        )

    def b_send(slot, part, u):
        for mask in sorted(masks, key=lambda m: (m & 1, m != SPLIT)):
            if source(mask, part)[0] == slot:
                b_copy(mask, part, u).start()

    def depth_of(mask):
        return bin(mask).count("1")

    def b_level(level, u, parts=(0, 1)):
        for part in parts:
            for mask in masks:
                if mask % 2 == 0 and depth_of(mask) == level:
                    b_wait(mask, part, u)
                    b_send(mask, part, u)

    depth = len(bits) - 1

    def level_one(o):
        for u in range(2):
            b_level(1, 2 * o + u)

    def level_rest(o):
        for level in range(2, depth + 1):
            for u in range(2):
                b_level(level, 2 * o + u)

    def head_norm(sums, gain, scale):
        meansq = jnp.mean(sums * sums, axis=-1, keepdims=True)
        return sums * lax.rsqrt(meansq + 1e-06) * gain * scale

    def project_chunk(first, count, own=False, between=None):
        units = pl.ds(first, count)

        def sums_of(j):
            if own:
                pltpu.make_async_copy(w_hbm.at[j], w_ref.at[j], w_sem.at[j]).wait()
            sums = jnp.dot(
                mod[units].reshape(count * half, model), w_ref[j], preferred_element_type=F32
            )
            return [sums[:, h * head:(h + 1) * head] for h in range(heads)]

        for h, sums in enumerate(sums_of(1)):
            keys = head_norm(sums, kg_ref[...], 1.0).astype(BF)
            kv[0, h, 0, units] = keys.reshape(count, half, head)
        for u in range(count):
            b_send(0, 0, first + u)
        for h, sums in enumerate(sums_of(2)):
            kv[1, h, 0, units] = sums.astype(BF).reshape(count, half, head)
        for u in range(count):
            b_send(0, 1, first + u)
        if between is not None:
            between()
        for h, sums in enumerate(sums_of(0)):
            queries = head_norm(sums, qg_ref[...], factor).astype(BF)
            q_ref[h, 0, units] = queries.reshape(count, half, head)
        for u in range(count):
            q_copy(first + u, theirs).start()

    def whole_chunk(o):
        project_chunk(2 * o, 2)

    for u in range(2):
        @pl.when(z < last)
        def _():
            a_right(2 * z + u).start()

        @pl.when(z > 0)
        def _():
            a_left(2 * z + u).start()

    def receive(k, u):
        @pl.when(z - k >= 0)
        def _():
            a_right(2 * (z - k) + u).wait_recv()

            @pl.when(z < last)
            def _():
                a_right(2 * (z - k) + u).start()

        @pl.when(z + k <= last)
        def _():
            a_left(2 * (z + k) + u).wait_recv()

            @pl.when(z > 0)
            def _():
                a_left(2 * (z + k) + u).start()

    def at_first(k, act):
        o = jnp.where(z >= k, z - k, z + k)

        @pl.when((z >= k) | (z + k <= last))
        def _():
            act(o)

    def at_second(k, act):
        @pl.when((z >= k) & (z + k <= last) & (k > 0))
        def _():
            act(z + k)

    with jax.named_scope("own"):
        project_chunk(2 * z, 2, own=True)
    receive(1, 0)
    if last > 1:
        receive(1, 1)

    def line_step(k, _):
        at_first(k - 1, level_one)
        at_first(k, whole_chunk)
        receive(k + 1, 0)
        at_second(k - 1, level_one)
        at_first(k - 1, level_rest)
        at_second(k, whole_chunk)

        @pl.when(k + 1 < last)
        def _():
            receive(k + 1, 1)

        at_second(k - 1, level_rest)
        return 0

    with jax.named_scope("line"):
        lax.fori_loop(1, last, line_step, 0)

    ends = (z == 0) | (z == last)
    far = last - z

    with jax.named_scope("far"):
        at_first(last - 1, level_one)

        def far_step(u, _):
            @pl.when(ends)
            def _():
                @pl.when(u == 1)
                def _():
                    receive(last, 1)

                def between():
                    @pl.when(u == 1)
                    def _():
                        b_level(1, 2 * far)

                project_chunk(2 * far + u, 1, between=between)

            @pl.when(u == 0)
            def _():
                at_second(last - 1, level_one)
                at_first(last - 1, level_rest)
                at_second(last - 1, level_rest)
            return 0

        lax.fori_loop(0, 2, far_step, 0)

        @pl.when(ends)
        def _():
            b_level(1, 2 * far + 1)
            for level in range(2, depth + 1):
                b_level(level, 2 * far)
                b_level(level, 2 * far + 1)

    def b_finish(u, _):
        for part in (0, 1):
            for mask in masks:
                if mask % 2 == 1:
                    b_wait(mask, part, u)
        q_copy(u, mine).wait_recv()
        return 0

    with jax.named_scope("b_finish"):
        lax.fori_loop(0, 2 * n_u, b_finish, 0)
        pltpu.make_async_copy(wo_hbm, wo_ref, w_sem.at[3]).wait()

    keys_all = n_blk * n_u * rows

    def order(i):
        return jnp.where(i % 2 == 0, i // 2, last - i // 2)

    def c_copy(o, src, sd, send, step):
        ref = att.at[o, src, :, pl.ds(pl.multiple_of(sd * cols, head), cols)]
        return pltpu.make_async_remote_copy(
            src_ref=ref, dst_ref=ref,
            send_sem=send.at[o, src, sd], recv_sem=rc.at[o, src, sd],
            device_id={"ulysses": z + step}, device_id_type=MESH,
        )

    def c_right(o, src, sd):
        return c_copy(o, src, sd, sc_r, 1)

    def c_left(o, src, sd):
        return c_copy(o, src, sd, sc_l, -1)

    def c_both(o, sd):
        @pl.when(z < last)
        def _():
            c_right(o, z, sd).start()

        @pl.when(z > 0)
        def _():
            c_left(o, z, sd).start()

    def x_copy(o, sd):
        return pltpu.make_async_remote_copy(
            src_ref=xatt.at[o],
            dst_ref=att.at[o, z, :, pl.ds(pl.multiple_of(sd * cols, head), cols)],
            send_sem=sx.at[o], recv_sem=rx.at[o],
            device_id={"blk": flip(SPLIT)}, device_id_type=MESH,
        )

    def d_copy(o, src):
        return pltpu.make_async_remote_copy(
            src_ref=stage.at[o], dst_ref=br.at[src],
            send_sem=sd.at[o], recv_sem=rd.at[src],
            device_id={"ulysses": o}, device_id_type=MESH,
        )

    def attend(o):
        chunk = pl.ds(2 * o, 2)
        for r in range(share):
            h = mine + r
            keys = kv[0, h].reshape(keys_all, head)
            values = kv[1, h].reshape(keys_all, head)
            queries = jnp.concatenate(
                [q_ref[h, p, chunk].reshape(rows, head) for p in range(2)], axis=0
            )
            scores = lax.dot_general(
                queries, keys, (((1,), (1,)), ((), ())), preferred_element_type=F32
            )
            powers = jnp.exp(scores - jnp.max(scores, axis=-1, keepdims=True))
            total = jnp.sum(powers, axis=-1, keepdims=True)
            numerator = jnp.dot(powers.astype(BF), values, preferred_element_type=F32)
            result = (numerator / total).astype(BF)
            place = pl.ds(pl.multiple_of(side * cols + r * head, head), head)
            att[o, z, :, place] = result[:rows]
            xatt[o, :, r * head:(r + 1) * head] = result[rows:]

    def pass_right(o, src):
        for sd in (side, 1 - side):
            c_right(o, src, sd).wait_recv()

            @pl.when(z < last)
            def _():
                c_right(o, src, sd).start()

    def pass_left(o, src):
        for sd in (side, 1 - side):
            c_left(o, src, sd).wait_recv()

            @pl.when(z > 0)
            def _():
                c_left(o, src, sd).start()

    low = z < n_u // 2

    def attend_step(t, _):
        @pl.when(t < n_u)
        def _():
            o = order(t)
            with jax.named_scope("attend"):
                attend(o)
            c_both(o, side)
            x_copy(o, side).start()

        @pl.when((t > 0) & (t <= n_u))
        def _():
            o = order(t - 1)
            x_copy(o, 1 - side).wait_recv()
            c_both(o, 1 - side)

        @pl.when((t > 1) & low & (z > 0))
        def _():
            pass_left(order(t - 2), z + 1)

        @pl.when((t > 1) & jnp.logical_not(low) & (z < last))
        def _():
            pass_right(order(t - 2), z - 1)

        return 0

    with jax.named_scope("attend_loop"):
        lax.fori_loop(0, n_u + 2, attend_step, 0)

    def mix_step(t, _):
        for k in range(last, 0, -1):
            i = t - k + 1
            held = (i >= 0) & (i < n_u)
            right_too = held & (z - k >= 0)
            left_too = held & (z + k <= last)
            if k == 1:
                right_too = right_too & (low | (z == last))
                left_too = left_too & (jnp.logical_not(low) | (z == 0))

            @pl.when(right_too)
            def _():
                pass_right(order(i), z - k)

            @pl.when(left_too)
            def _():
                pass_left(order(i), z + k)

        @pl.when(t >= last - 1)
        def _():
            o = order(t - last + 1)
            total = jnp.zeros((rows, width), F32)
            for src in range(n_u):
                total += jnp.dot(
                    att[o, src], wo_ref[src * width:(src + 1) * width, :],
                    preferred_element_type=F32,
                )

            @pl.when(o == z)
            def _():
                br[z] = total.astype(BF)

            @pl.when(o != z)
            def _():
                stage[o] = total.astype(BF)
                d_copy(o, z).start()

        return 0

    with jax.named_scope("mix_loop"):
        lax.fori_loop(0, n_u + last - 1, mix_step, 0)

    with jax.named_scope("final"):
        for src in range(n_u):
            @pl.when(src != z)
            def _():
                d_copy(src, src).wait_recv()

            at = slice(src * width, (src + 1) * width)
            out_ref[:, at] = (
                tok_ref[:, at].astype(F32) + gate_ref[:, at] * br[src].astype(F32)
            ).astype(BF)

    def finish(s, _):
        for u in range(2):
            @pl.when((s <= z) & (z < last))
            def _():
                a_right(2 * s + u).wait_send()

            @pl.when((s >= z) & (z > 0))
            def _():
                a_left(2 * s + u).wait_send()

        for src in range(n_u):
            for sd_of in range(2):
                @pl.when((src <= z) & (z < last))
                def _():
                    c_right(s, src, sd_of).wait_send()

                @pl.when((src >= z) & (z > 0))
                def _():
                    c_left(s, src, sd_of).wait_send()

        @pl.when(s != z)
        def _():
            d_copy(s, z).wait_send()

        x_copy(s, side).wait_send()
        for u in range(2):
            q_copy(2 * s + u, theirs).wait_send()
        for part in (0, 1):
            for mask in masks:
                for u in range(2):
                    b_copy(mask, part, 2 * s + u).wait_send()
        return 0

    with jax.named_scope("finish"):
        lax.fori_loop(0, n_u, finish, 0)


def local(n_u, n_blk, tokens, mod_shift, mod_scale, mod_gate, qkv_weight, query_gain, key_gain, out_weight):
    rows, model = tokens.shape
    width = qkv_weight.shape[2]
    head = query_gain.shape[0]
    heads = width // head
    vmem = pl.BlockSpec(memory_space=pltpu.VMEM)
    hbm = pl.BlockSpec(memory_space=pl.ANY)
    dma = pltpu.SemaphoreType.DMA
    split = heads % 2 == 0 and n_blk % (2 * SPLIT) == 0
    buffers = [
        pltpu.VMEM(qkv_weight.shape, BF),
        pltpu.VMEM(out_weight.shape, BF),
        pltpu.VMEM((2 * n_u, rows // 2, model), BF),
    ]
    line_sems = [dma((4,)), dma((2 * n_u,)), dma((2 * n_u,)), dma((2 * n_u,))]
    block_sems = [dma((n_blk, 2, 2 * n_u)), dma((n_blk, 2, 2 * n_u))]
    keys = pltpu.VMEM((2, heads, n_blk, 2 * n_u, rows // 2, head), BF)
    attended = pltpu.VMEM((n_u, n_u, rows, width), BF)
    mixed = pltpu.VMEM((n_u, rows, width), BF)
    if split:
        body = split_kernel
        scratch = buffers + [
            pltpu.VMEM((heads, 2, 2 * n_u, rows // 2, head), BF), keys,
            attended, pltpu.VMEM((n_u, rows, width // 2), BF), mixed, mixed,
        ] + line_sems + block_sems + [
            dma((2 * n_u,)), dma((2 * n_u,)), dma((n_u,)), dma((n_u,)),
            dma((n_u, n_u, 2)), dma((n_u, n_u, 2)), dma((n_u, n_u, 2)),
            dma((n_u,)), dma((n_u,)),
        ]
    else:
        body = kernel
        scratch = buffers + [
            pltpu.VMEM((heads, 2 * n_u, rows // 2, head), BF), keys,
            attended, mixed, mixed,
        ] + line_sems + block_sems + [
            dma((n_u, n_u)), dma((n_u, n_u)), dma((n_u, n_u)),
            dma((n_u,)), dma((n_u,)),
        ]
    return pl.pallas_call(
        functools.partial(body, n_u, n_blk),
        out_shape=jax.ShapeDtypeStruct((rows, model), BF),
        in_specs=[vmem, vmem, vmem, vmem, hbm, vmem, vmem, hbm],
        out_specs=vmem,
        scratch_shapes=scratch,
        compiler_params=pltpu.CompilerParams(
            collective_id=0, has_side_effects=True, vmem_limit_bytes=66_000_000
        ),
    )(
        tokens, mod_shift[None], mod_scale[None], mod_gate[None],
        qkv_weight, query_gain[None], key_gain[None], out_weight,
    )


def solution(mesh):
    in_specs = (
        P(("blk", "ulysses"), None), P(), P(), P(),
        P(None, None, "ulysses"), P(), P(), P(None, "ulysses"),
    )
    out_specs = P(("blk", "ulysses"), None)
    body = functools.partial(local, mesh.shape["ulysses"], mesh.shape["blk"])
    return jax.shard_map(body, mesh=mesh, in_specs=in_specs, out_specs=out_specs, check_vma=False)
```

```python
import functools
import math

import jax
import jax.numpy as jnp
from jax import lax
from jax.experimental import pallas as pl
from jax.experimental.pallas import tpu as pltpu
from jax.sharding import PartitionSpec as P

MESH = pl.DeviceIdType.MESH
BF = jnp.bfloat16
F32 = jnp.float32
SPLIT = 2


def highest_bit(mask):
    return 1 << (mask.bit_length() - 1)


def lowest_bit(mask):
    return mask & -mask


def source_slot(mask, part):
    if mask & 1:
        return mask - 1, 1
    bit = highest_bit(mask) if part == 0 else lowest_bit(mask)
    return mask - bit, bit


def kernel(
    n_u, n_blk,
    tok_ref, shift_ref, scale_ref, gate_ref, w_hbm, qg_ref, kg_ref, wo_hbm, out_ref,
    w_ref, wo_ref, mod, q_ref, kv, att, stage, br,
    w_sem, sa_r, sa_l, ra, sb, rb, sc_r, sc_l, rc, sd, rd,
):
    z = lax.axis_index("ulysses")
    b = lax.axis_index("blk")
    rows, model = tok_ref.shape
    head = qg_ref.shape[1]
    width = w_ref.shape[2]
    heads = width // head
    factor = 1.0 / math.sqrt(head)
    last = n_u - 1
    half = rows // 2
    bits = [1 << i for i in range(n_blk.bit_length() - 1)]
    pair = 2 if heads % 2 == 0 else heads
    tile = pair * head

    for j in (1, 2, 0):
        pltpu.make_async_copy(w_hbm.at[j], w_ref.at[j], w_sem.at[j]).start()
    pltpu.make_async_copy(wo_hbm, wo_ref, w_sem.at[3]).start()

    def flip(bit):
        return b + (1 - 2 * ((b // bit) % 2)) * bit

    barrier = pltpu.get_barrier_semaphore()
    for d in range(1, n_u):
        pl.semaphore_signal(
            barrier, inc=1, device_id={"ulysses": (z + d) % n_u}, device_id_type=MESH
        )
    for bit in bits:
        pl.semaphore_signal(barrier, inc=1, device_id={"blk": flip(bit)}, device_id_type=MESH)

    wide = tok_ref[...].astype(F32)
    center = jnp.mean(wide, axis=-1, keepdims=True)
    spread = jnp.mean((wide - center) ** 2, axis=-1, keepdims=True)
    normed = (wide - center) * lax.rsqrt(spread + 1e-06)
    modulated = (normed * (1.0 + scale_ref[...]) + shift_ref[...]).astype(BF)
    mod[pl.ds(2 * z, 2)] = modulated.reshape(2, half, model)

    pl.semaphore_wait(barrier, n_u - 1 + len(bits))

    def line_copy(buf, index, send, recv, step):
        return pltpu.make_async_remote_copy(
            src_ref=buf.at[index], dst_ref=buf.at[index],
            send_sem=send.at[index], recv_sem=recv.at[index],
            device_id={"ulysses": z + step}, device_id_type=MESH,
        )

    def a_right(o):
        return line_copy(mod, o, sa_r, ra, 1)

    def a_left(o):
        return line_copy(mod, o, sa_l, ra, -1)

    def b_copy(mask, part, s):
        slot, bit = source_slot(mask, part)
        return pltpu.make_async_remote_copy(
            src_ref=kv.at[part, :, slot, s], dst_ref=kv.at[part, :, mask, s],
            send_sem=sb.at[mask, part, s], recv_sem=rb.at[mask, part, s],
            device_id={"blk": flip(bit)}, device_id_type=MESH,
        )

    masks = range(1, n_blk)

    def b_send(slot, part, s):
        for mask in sorted(masks, key=lambda m: m & 1):
            if source_slot(mask, part)[0] == slot:
                b_copy(mask, part, s).start()

    def b_level(level, s):
        for part in (0, 1):
            for mask in masks:
                if mask % 2 == 0 and bin(mask).count("1") == level:
                    b_copy(mask, part, s).wait_recv()
                    b_send(mask, part, s)

    levels = range(1, len(bits))

    def head_norm(sums, gain, scale):
        meansq = jnp.mean(sums * sums, axis=-1, keepdims=True)
        return sums * lax.rsqrt(meansq + 1e-06) * gain * scale

    def project(j, first, count, put):
        def body(i, _):
            start = pl.multiple_of(i * tile, tile)
            sums = jnp.dot(
                mod[pl.ds(first, count)].reshape(count * half, model),
                w_ref[j, :, pl.ds(start, tile)],
                preferred_element_type=F32,
            )
            for e in range(pair):
                put(i * pair + e, sums[:, e * head:(e + 1) * head])
            return 0

        lax.fori_loop(0, heads // pair, body, 0)

    def project_chunk(first, count, own=False):
        units = pl.ds(first, count)

        def ready(j):
            if own:
                pltpu.make_async_copy(w_hbm.at[j], w_ref.at[j], w_sem.at[j]).wait()

        def put_key(h, sums):
            keys = head_norm(sums, kg_ref[...], 1.0).astype(BF)
            kv[0, h, 0, units] = keys.reshape(count, half, head)

        def put_value(h, sums):
            kv[1, h, 0, units] = sums.astype(BF).reshape(count, half, head)

        def put_query(h, sums):
            queries = head_norm(sums, qg_ref[...], factor).astype(BF)
            q_ref[h, units] = queries.reshape(count, half, head)

        ready(1)
        project(1, first, count, put_key)
        for u in range(count):
            b_send(0, 0, first + u)
        ready(2)
        project(2, first, count, put_value)
        for u in range(count):
            b_send(0, 1, first + u)
        ready(0)
        project(0, first, count, put_query)

    for u in range(2):
        @pl.when(z < last)
        def _():
            a_right(2 * z + u).start()

        @pl.when(z > 0)
        def _():
            a_left(2 * z + u).start()

    project_chunk(2 * z, 2, own=True)

    def at_distance(k, act):
        for side in (-1, 1):
            o = z + side * k

            @pl.when((o >= 0) & (o <= last))
            def _():
                act(o)

    def pass_levels(which):
        def act(o):
            for level in which:
                for u in range(2):
                    b_level(level, 2 * o + u)
        return act

    def receive(k):
        for u in range(2):
            @pl.when(z - k >= 0)
            def _():
                a_right(2 * (z - k) + u).wait_recv()

                @pl.when(z < last)
                def _():
                    a_right(2 * (z - k) + u).start()

            @pl.when(z + k <= last)
            def _():
                a_left(2 * (z + k) + u).wait_recv()

                @pl.when(z > 0)
                def _():
                    a_left(2 * (z + k) + u).start()

    def previous(k, which):
        if isinstance(k, int) and k == 1:
            pass_levels(which)(z)
        else:
            at_distance(k - 1, pass_levels(which))

    for k in range(1, last):
        receive(k)
        previous(k, levels[:1])
        at_distance(k, lambda o: project_chunk(2 * o, 2))
        previous(k, levels[1:])

    ends = (z == 0) | (z == last)
    far = last - z

    def far_half(u):
        @pl.when(ends)
        def _():
            @pl.when(z == 0)
            def _():
                a_left(2 * far + u).wait_recv()

            @pl.when(z > 0)
            def _():
                a_right(2 * far + u).wait_recv()

            project_chunk(2 * far + u, 1)

    def far_levels(u, which):
        @pl.when(ends)
        def _():
            for level in which:
                b_level(level, 2 * far + u)

    previous(last, levels[:1])
    far_half(0)
    previous(last, levels[1:])
    far_levels(0, levels[:1])
    far_half(1)
    far_levels(0, levels[1:])
    far_levels(1, levels)

    def b_finish(s, _):
        for part in (0, 1):
            for mask in masks:
                if mask % 2 == 1:
                    b_copy(mask, part, s).wait_recv()
        return 0

    lax.fori_loop(0, 2 * n_u, b_finish, 0)
    pltpu.make_async_copy(wo_hbm, wo_ref, w_sem.at[3]).wait()

    keys_all = n_blk * n_u * rows

    def order(i):
        return jnp.where(i % 2 == 0, i // 2, last - i // 2)

    def c_right(o, src):
        return pltpu.make_async_remote_copy(
            src_ref=att.at[o, src], dst_ref=att.at[o, src],
            send_sem=sc_r.at[o, src], recv_sem=rc.at[o, src],
            device_id={"ulysses": z + 1}, device_id_type=MESH,
        )

    def c_left(o, src):
        return pltpu.make_async_remote_copy(
            src_ref=att.at[o, src], dst_ref=att.at[o, src],
            send_sem=sc_l.at[o, src], recv_sem=rc.at[o, src],
            device_id={"ulysses": z - 1}, device_id_type=MESH,
        )

    def d_copy(o, src):
        return pltpu.make_async_remote_copy(
            src_ref=stage.at[o], dst_ref=br.at[src],
            send_sem=sd.at[o], recv_sem=rd.at[src],
            device_id={"ulysses": o}, device_id_type=MESH,
        )

    group = 2 if n_u % 2 == 0 else 1

    def attend(chunks):
        for h in range(heads):
            keys = kv[0, h].reshape(keys_all, head)
            values = kv[1, h].reshape(keys_all, head)
            queries = jnp.concatenate(
                [q_ref[h, pl.ds(2 * o, 2)].reshape(rows, head) for o in chunks], axis=0
            )
            scores = lax.dot_general(
                queries, keys, (((1,), (1,)), ((), ())), preferred_element_type=F32
            )
            powers = jnp.exp(scores - jnp.max(scores, axis=-1, keepdims=True))
            total = jnp.sum(powers, axis=-1, keepdims=True)
            numerator = jnp.dot(powers.astype(BF), values, preferred_element_type=F32)
            result = (numerator / total).astype(BF)
            for g, o in enumerate(chunks):
                att[o, z, :, h * head:(h + 1) * head] = result[g * rows:(g + 1) * rows]

    def pass_right(o, src):
        c_right(o, src).wait_recv()

        @pl.when(z < last)
        def _():
            c_right(o, src).start()

    def pass_left(o, src):
        c_left(o, src).wait_recv()

        @pl.when(z > 0)
        def _():
            c_left(o, src).start()

    low = z < n_u // 2

    def attend_step(t, _):
        @pl.when(t < n_u // group)
        def _():
            chunks = [order(group * t + g) for g in range(group)]
            attend(chunks)
            for o in chunks:
                @pl.when(z < last)
                def _():
                    c_right(o, z).start()

                @pl.when(z > 0)
                def _():
                    c_left(o, z).start()

        for g in range(group):
            @pl.when((t > 0) & low & (z > 0))
            def _():
                pass_left(order(group * (t - 1) + g), z + 1)

            @pl.when((t > 0) & jnp.logical_not(low) & (z < last))
            def _():
                pass_right(order(group * (t - 1) + g), z - 1)

        return 0

    lax.fori_loop(0, n_u // group + 1, attend_step, 0)

    def mix_step(t, _):
        for k in range(last, 0, -1):
            i = t - k + 1
            held = (i >= 0) & (i < n_u)
            right_too = held & (z - k >= 0)
            left_too = held & (z + k <= last)
            if k == 1:
                right_too = right_too & (low | (z == last))
                left_too = left_too & (jnp.logical_not(low) | (z == 0))

            @pl.when(right_too)
            def _():
                pass_right(order(i), z - k)

            @pl.when(left_too)
            def _():
                pass_left(order(i), z + k)

        @pl.when(t >= last - 1)
        def _():
            o = order(t - last + 1)
            total = jnp.zeros((rows, width), F32)
            for src in range(n_u):
                total += jnp.dot(
                    att[o, src], wo_ref[src * width:(src + 1) * width, :],
                    preferred_element_type=F32,
                )

            @pl.when(o == z)
            def _():
                br[z] = total.astype(BF)

            @pl.when(o != z)
            def _():
                stage[o] = total.astype(BF)
                d_copy(o, z).start()

        return 0

    lax.fori_loop(0, n_u + last - 1, mix_step, 0)

    for src in range(n_u):
        @pl.when(src != z)
        def _():
            d_copy(src, src).wait_recv()

        cols = slice(src * width, (src + 1) * width)
        out_ref[:, cols] = (
            tok_ref[:, cols].astype(F32) + gate_ref[:, cols] * br[src].astype(F32)
        ).astype(BF)

    def finish(s, _):
        for u in range(2):
            @pl.when((s <= z) & (z < last))
            def _():
                a_right(2 * s + u).wait_send()

            @pl.when((s >= z) & (z > 0))
            def _():
                a_left(2 * s + u).wait_send()

        for src in range(n_u):
            @pl.when((src <= z) & (z < last))
            def _():
                c_right(s, src).wait_send()

            @pl.when((src >= z) & (z > 0))
            def _():
                c_left(s, src).wait_send()

        @pl.when(s != z)
        def _():
            d_copy(s, z).wait_send()

        for part in (0, 1):
            for mask in masks:
                for u in range(2):
                    b_copy(mask, part, 2 * s + u).wait_send()
        return 0

    lax.fori_loop(0, n_u, finish, 0)


def split_kernel(
    n_u, n_blk,
    tok_hbm, shift_hbm, scale_hbm, gate_hbm, w_hbm, qg_ref, kg_ref, wo_hbm, out_ref,
    w_ref, wo_ref, mod, q_ref, kv, att, xatt, pair_ref, stage, br,
    tok_ref, shift_ref, scale_ref, gate_ref, in_sem,
    w_sem, sa_r, sa_l, ra, sb, rb, sq, rq, sx, rx, sc_r, sc_l, rc, sd, rd,
):
    z = lax.axis_index("ulysses")
    b = lax.axis_index("blk")
    rows, model = tok_ref.shape
    head = qg_ref.shape[1]
    width = w_ref.shape[2]
    heads = width // head
    share = heads // 2
    cols = share * head
    factor = 1.0 / math.sqrt(head)
    last = n_u - 1
    half = rows // 2
    bits = [1 << i for i in range(n_blk.bit_length() - 1)]
    masks = range(1, n_blk)
    side = (b // SPLIT) % 2
    mine = side * share
    theirs = (1 - side) * share

    def flip(bit):
        return b + (1 - 2 * ((b // bit) % 2)) * bit

    barrier = pltpu.get_barrier_semaphore()
    for d in range(1, n_u):
        pl.semaphore_signal(
            barrier, inc=1, device_id={"ulysses": (z + d) % n_u}, device_id_type=MESH
        )
    for bit in bits:
        pl.semaphore_signal(barrier, inc=1, device_id={"blk": flip(bit)}, device_id_type=MESH)

    inputs = [
        pltpu.make_async_copy(src, dst, in_sem.at[i])
        for i, (src, dst) in enumerate((
            (tok_hbm, tok_ref), (shift_hbm, shift_ref), (scale_hbm, scale_ref), (gate_hbm, gate_ref),
        ))
    ]
    for copy in inputs:
        copy.start()
    for copy in inputs:
        copy.wait()
    for j in (1, 2, 0):
        pltpu.make_async_copy(w_hbm.at[j], w_ref.at[j], w_sem.at[j]).start()
    pltpu.make_async_copy(wo_hbm, wo_ref, w_sem.at[3]).start()

    wide = tok_ref[...].astype(F32)
    center = jnp.mean(wide, axis=-1, keepdims=True)
    spread = jnp.mean((wide - center) ** 2, axis=-1, keepdims=True)
    normed = (wide - center) * lax.rsqrt(spread + 1e-06)
    modulated = (normed * (1.0 + scale_ref[...]) + shift_ref[...]).astype(BF)
    mod[pl.ds(2 * z, 2)] = modulated.reshape(2, half, model)

    with jax.named_scope("barrier"):
        pl.semaphore_wait(barrier, n_u - 1 + len(bits))

    def line_copy(buf, index, send, recv, step):
        return pltpu.make_async_remote_copy(
            src_ref=buf.at[index], dst_ref=buf.at[index],
            send_sem=send.at[index], recv_sem=recv.at[index],
            device_id={"ulysses": z + step}, device_id_type=MESH,
        )

    def a_right(o):
        return line_copy(mod, o, sa_r, ra, 1)

    def a_left(o):
        return line_copy(mod, o, sa_l, ra, -1)

    def source(mask, part):
        if mask & 1:
            return mask - 1, 1
        if mask == SPLIT:
            return 0, SPLIT
        rest = mask & ~SPLIT
        bit = highest_bit(rest) if part == 0 else lowest_bit(rest)
        return mask - bit, bit

    def b_copy(mask, part, u):
        slot, bit = source(mask, part)
        own = pl.ds(theirs if bit == SPLIT else mine, share)
        return pltpu.make_async_remote_copy(
            src_ref=kv.at[part, own, slot, u], dst_ref=kv.at[part, own, mask, u],
            send_sem=sb.at[mask, part, u], recv_sem=rb.at[mask, part, u],
            device_id={"blk": flip(bit)}, device_id_type=MESH,
        )

    def b_wait(mask, part, u):
        here = kv.at[part, pl.ds(mine, share), mask, u]
        pltpu.make_async_remote_copy(
            src_ref=here, dst_ref=here,
            send_sem=sb.at[mask, part, u], recv_sem=rb.at[mask, part, u],
            device_id={"blk": flip(source(mask, part)[1])}, device_id_type=MESH,
        ).wait_recv()

    def q_copy(u, first):
        heads_of = pl.ds(first, share)
        return pltpu.make_async_remote_copy(
            src_ref=q_ref.at[heads_of, 0, u], dst_ref=q_ref.at[heads_of, 1, u],
            send_sem=sq.at[u], recv_sem=rq.at[u],
            device_id={"blk": flip(SPLIT)}, device_id_type=MESH,
        )

    def b_send(slot, part, u):
        for mask in sorted(masks, key=lambda m: (m & 1, m != SPLIT)):
            if source(mask, part)[0] == slot:
                b_copy(mask, part, u).start()

    def depth_of(mask):
        return bin(mask).count("1")

    def b_level(level, u, parts=(0, 1)):
        for part in parts:
            for mask in masks:
                if mask % 2 == 0 and depth_of(mask) == level:
                    b_wait(mask, part, u)
                    b_send(mask, part, u)

    depth = len(bits) - 1

    def level_one(o):
        for u in range(2):
            b_level(1, 2 * o + u)

    def level_rest(o):
        for level in range(2, depth + 1):
            for u in range(2):
                b_level(level, 2 * o + u)

    def head_norm(sums, gain, scale):
        meansq = jnp.mean(sums * sums, axis=-1, keepdims=True)
        return sums * lax.rsqrt(meansq + 1e-06) * gain * scale

    def project(starts, count, own=False, between=None):
        size = count * half

        def sums_of(j):
            if own:
                pltpu.make_async_copy(w_hbm.at[j], w_ref.at[j], w_sem.at[j]).wait()
            tokens = [mod[pl.ds(first, count)].reshape(size, model) for first in starts]
            sums = jnp.dot(
                jnp.concatenate(tokens, axis=0), w_ref[j], preferred_element_type=F32
            )
            return [sums[:, h * head:(h + 1) * head] for h in range(heads)]

        def put(value, at):
            for i, first in enumerate(starts):
                at(pl.ds(first, count), value[i * size:(i + 1) * size].reshape(count, half, head))

        def send(act):
            for first in starts:
                for u in range(count):
                    act(first + u)

        for h, sums in enumerate(sums_of(1)):
            def put_keys(units, part):
                kv[0, h, 0, units] = part
            put(head_norm(sums, kg_ref[...], 1.0).astype(BF), put_keys)
        send(lambda u: b_send(0, 0, u))
        for h, sums in enumerate(sums_of(2)):
            def put_values(units, part):
                kv[1, h, 0, units] = part
            put(sums.astype(BF), put_values)
        send(lambda u: b_send(0, 1, u))
        if between is not None:
            between()
        for h, sums in enumerate(sums_of(0)):
            def put_queries(units, part):
                q_ref[h, 0, units] = part
            put(head_norm(sums, qg_ref[...], factor).astype(BF), put_queries)
        send(lambda u: q_copy(u, theirs).start())

    for u in range(2):
        @pl.when(z < last)
        def _():
            a_right(2 * z + u).start()

        @pl.when(z > 0)
        def _():
            a_left(2 * z + u).start()

    def receive(k, u):
        @pl.when(z - k >= 0)
        def _():
            a_right(2 * (z - k) + u).wait_recv()

            @pl.when(z < last)
            def _():
                a_right(2 * (z - k) + u).start()

        @pl.when(z + k <= last)
        def _():
            a_left(2 * (z + k) + u).wait_recv()

            @pl.when(z > 0)
            def _():
                a_left(2 * (z + k) + u).start()

    def at_each(k, act):
        @pl.when(z >= k)
        def _():
            act(z - k)

        @pl.when((z + k <= last) & (k > 0))
        def _():
            act(z + k)

    def project_at(k, between):
        two = (z >= k) & (z + k <= last)

        @pl.when(two)
        def _():
            project([2 * (z - k), 2 * (z + k)], 2, between=between)

        @pl.when(jnp.logical_not(two) & ((z >= k) | (z + k <= last)))
        def _():
            project([2 * jnp.where(z >= k, z - k, z + k)], 2, between=between)

    with jax.named_scope("own"):
        project([2 * z], 2, own=True)
    receive(1, 0)
    level_one(z)
    if last > 1:
        receive(1, 1)

    def line_step(k, _):
        with jax.named_scope("project"):
            project_at(k, lambda: at_each(k - 1, level_rest))
        receive(k + 1, 0)
        at_each(k, level_one)

        @pl.when(k + 1 < last)
        def _():
            receive(k + 1, 1)

        return 0

    with jax.named_scope("line"):
        lax.fori_loop(1, last, line_step, 0)

    ends = (z == 0) | (z == last)
    far = last - z

    with jax.named_scope("far"):
        @pl.when(jnp.logical_not(ends))
        def _():
            at_each(last - 1, level_rest)

        def far_step(u, _):
            @pl.when(u == 1)
            def _():
                receive(last, 1)

            def between():
                @pl.when(u == 0)
                def _():
                    at_each(last - 1, level_rest)

                @pl.when(u == 1)
                def _():
                    b_level(1, 2 * far)

            with jax.named_scope("project_half"):
                project([2 * far + u], 1, between=between)
            return 0

        @pl.when(ends)
        def _():
            lax.fori_loop(0, 2, far_step, 0)
            b_level(1, 2 * far + 1)
            for level in range(2, depth + 1):
                b_level(level, 2 * far)
                b_level(level, 2 * far + 1)

    def b_finish(u, _):
        for part in (0, 1):
            for mask in masks:
                if mask % 2 == 1:
                    b_wait(mask, part, u)
        q_copy(u, mine).wait_recv()
        return 0

    with jax.named_scope("b_finish"):
        lax.fori_loop(0, 2 * n_u, b_finish, 0)
        pltpu.make_async_copy(wo_hbm, wo_ref, w_sem.at[3]).wait()

    keys_all = n_blk * n_u * rows

    def order(i, rightward):
        inner = n_u - 2
        low_end = (i == inner) == rightward
        return jnp.where(i < inner, i + 1, jnp.where(low_end, 0, last))

    def c_copy(o, src, sd, send, step):
        ref = att.at[o, src, :, pl.ds(pl.multiple_of(sd * cols, head), cols)]
        return pltpu.make_async_remote_copy(
            src_ref=ref, dst_ref=ref,
            send_sem=send.at[o, src, sd], recv_sem=rc.at[o, src, sd],
            device_id={"ulysses": z + step}, device_id_type=MESH,
        )

    def c_right(o, src, sd):
        return c_copy(o, src, sd, sc_r, 1)

    def c_left(o, src, sd):
        return c_copy(o, src, sd, sc_l, -1)

    low = z < n_u // 2

    def c_send(t, sd):
        o = order(t, low)

        def start(right, chunk):
            @pl.when(right & (z < last))
            def _():
                c_right(chunk, z, sd).start()

            @pl.when(jnp.logical_not(right) & (z > 0))
            def _():
                c_left(chunk, z, sd).start()

        start(low, o)

        @pl.when(t != n_u - 2)
        def _():
            start(jnp.logical_not(low), o)

        @pl.when(t == n_u - 1)
        def _():
            start(jnp.logical_not(low), order(t - 1, low))

    def x_copy(o, sd):
        return pltpu.make_async_remote_copy(
            src_ref=xatt.at[o],
            dst_ref=att.at[o, z, :, pl.ds(pl.multiple_of(sd * cols, head), cols)],
            send_sem=sx.at[o], recv_sem=rx.at[o],
            device_id={"blk": flip(SPLIT)}, device_id_type=MESH,
        )

    def d_copy(o, src):
        return pltpu.make_async_remote_copy(
            src_ref=stage.at[o], dst_ref=br.at[src],
            send_sem=sd.at[o], recv_sem=rd.at[src],
            device_id={"ulysses": o}, device_id_type=MESH,
        )

    def attend(t):
        first, second = t == 0, t == n_u - 1
        groups = (
            (first, order(jnp.where(first, 0, t - 1), low)),
            (jnp.logical_not(second), order(jnp.where(second, t, t + 1), low)),
        )
        for r in range(share):
            h = mine + r
            keys = kv[0, h].reshape(keys_all, head)
            values = kv[1, h].reshape(keys_all, head)
            queries = jnp.concatenate([
                q_ref[h, jnp.where(away, 1, 0), pl.ds(2 * o, 2)].reshape(rows, head)
                for away, o in groups
            ], axis=0)
            scores = lax.dot_general(
                queries, keys, (((1,), (1,)), ((), ())), preferred_element_type=F32
            )
            powers = jnp.exp(scores - jnp.max(scores, axis=-1, keepdims=True))
            total = jnp.sum(powers, axis=-1, keepdims=True)
            numerator = jnp.dot(powers.astype(BF), values, preferred_element_type=F32)
            pair_ref[:, r * head:(r + 1) * head] = (numerator / total).astype(BF)
        for g, (away, o) in enumerate(groups):
            @pl.when(away)
            def _():
                xatt[o] = pair_ref[g * rows:(g + 1) * rows]
                x_copy(o, side).start()

            @pl.when(jnp.logical_not(away))
            def _():
                place = pl.ds(pl.multiple_of(side * cols, head), cols)
                att[o, z, :, place] = pair_ref[g * rows:(g + 1) * rows]

        @pl.when(t > 0)
        def _():
            c_send(t - 1, side)

        @pl.when(second)
        def _():
            c_send(t, side)

    def pass_on(right, o, src, sd):
        copy = c_right(o, src, sd) if right else c_left(o, src, sd)
        copy.wait_recv()

        @pl.when((z < last) if right else (z > 0))
        def _():
            copy.start()

    def pass_when(when, right, i, src):
        @pl.when(when & (i >= 0) & (i < n_u))
        def _():
            pass_on(right, order(i, right), src, side)

        @pl.when(when & (i >= 1) & (i <= n_u))
        def _():
            pass_on(right, order(i - 1, right), src, 1 - side)

    def x_step(t):
        x_copy(order(t, low), 1 - side).wait_recv()
        c_send(t, 1 - side)

    def attend_step(t, _):
        with jax.named_scope("attend"):
            attend(t)

        @pl.when(t > 1)
        def _():
            x_step(t - 2)

        return 0

    with jax.named_scope("attend_loop"):
        lax.fori_loop(0, n_u, attend_step, 0)
        for t in range(max(n_u - 2, 0), n_u):
            x_step(t)

    def near_step(i, _):
        pass_when(low & (z > 0), False, i, z + 1)
        pass_when(jnp.logical_not(low) & (z < last), True, i, z - 1)
        return 0

    with jax.named_scope("near_loop"):
        lax.fori_loop(0, n_u + 1, near_step, 0)

    gap = 2
    reach = jnp.where(ends, last, jnp.maximum(z, last - z))

    def mix(i, _):
        o = order(i, jnp.logical_not(low))
        with jax.named_scope("mix"):
            total = jnp.zeros((rows, width), F32)
            for src in range(n_u):
                total += jnp.dot(
                    att[o, src], wo_ref[src * width:(src + 1) * width, :],
                    preferred_element_type=F32,
                )

        @pl.when(o == z)
        def _():
            br[z] = total.astype(BF)

        @pl.when(o != z)
        def _():
            stage[o] = total.astype(BF)
            d_copy(o, z).start()

        return 0

    def mix_step(t, _):
        for k in range(1, last + 1):
            i = t - gap * (k - 1)
            if k == 1:
                pass_when((z >= k) & (low | (z == last)), True, i, z - k)
                pass_when((z + k <= last) & (jnp.logical_not(low) | (z == 0)), False, i, z + k)
            else:
                pass_when(z >= k, True, i, z - k)
                pass_when(z + k <= last, False, i, z + k)

        i = t - gap * (reach - 1) - 1
        held = (i >= 0) & (i < n_u) & (ends | (i != n_u - 2))
        both = jnp.logical_not(ends) & (i == n_u - 1)
        lax.fori_loop(jnp.where(both, i - 1, i), jnp.where(held, i + 1, i), mix, 0)
        return 0

    with jax.named_scope("mix_loop"):
        lax.fori_loop(0, n_u + gap * (last - 1) + 1, mix_step, 0)

    with jax.named_scope("final"):
        for src in range(n_u):
            @pl.when(src != z)
            def _():
                d_copy(src, src).wait_recv()

            at = slice(src * width, (src + 1) * width)
            out_ref[:, at] = (
                tok_ref[:, at].astype(F32) + gate_ref[:, at] * br[src].astype(F32)
            ).astype(BF)

    def finish(s, _):
        for u in range(2):
            @pl.when((s <= z) & (z < last))
            def _():
                a_right(2 * s + u).wait_send()

            @pl.when((s >= z) & (z > 0))
            def _():
                a_left(2 * s + u).wait_send()

        for src in range(n_u):
            for sd_of in range(2):
                @pl.when((src <= z) & (z < last))
                def _():
                    c_right(s, src, sd_of).wait_send()

                @pl.when((src >= z) & (z > 0))
                def _():
                    c_left(s, src, sd_of).wait_send()

        @pl.when(s != z)
        def _():
            d_copy(s, z).wait_send()

        x_copy(s, side).wait_send()
        for u in range(2):
            q_copy(2 * s + u, theirs).wait_send()
        for part in (0, 1):
            for mask in masks:
                for u in range(2):
                    b_copy(mask, part, 2 * s + u).wait_send()
        return 0

    with jax.named_scope("finish"):
        lax.fori_loop(0, n_u, finish, 0)


def local(n_u, n_blk, tokens, mod_shift, mod_scale, mod_gate, qkv_weight, query_gain, key_gain, out_weight):
    rows, model = tokens.shape
    width = qkv_weight.shape[2]
    head = query_gain.shape[0]
    heads = width // head
    vmem = pl.BlockSpec(memory_space=pltpu.VMEM)
    hbm = pl.BlockSpec(memory_space=pl.ANY)
    dma = pltpu.SemaphoreType.DMA
    split = heads % 2 == 0 and n_blk % (2 * SPLIT) == 0
    buffers = [
        pltpu.VMEM(qkv_weight.shape, BF),
        pltpu.VMEM(out_weight.shape, BF),
        pltpu.VMEM((2 * n_u, rows // 2, model), BF),
    ]
    line_sems = [dma((4,)), dma((2 * n_u,)), dma((2 * n_u,)), dma((2 * n_u,))]
    block_sems = [dma((n_blk, 2, 2 * n_u)), dma((n_blk, 2, 2 * n_u))]
    keys = pltpu.VMEM((2, heads, n_blk, 2 * n_u, rows // 2, head), BF)
    attended = pltpu.VMEM((n_u, n_u, rows, width), BF)
    mixed = pltpu.VMEM((n_u, rows, width), BF)
    row = pltpu.VMEM((1, model), F32)
    early = hbm if split else vmem
    if split:
        body = split_kernel
        scratch = buffers + [
            pltpu.VMEM((heads, 2, 2 * n_u, rows // 2, head), BF), keys,
            attended, pltpu.VMEM((n_u, rows, width // 2), BF),
            pltpu.VMEM((2 * rows, width // 2), BF), mixed, mixed,
            pltpu.VMEM((rows, model), BF), row, row, row, dma((4,)),
        ] + line_sems + block_sems + [
            dma((2 * n_u,)), dma((2 * n_u,)), dma((n_u,)), dma((n_u,)),
            dma((n_u, n_u, 2)), dma((n_u, n_u, 2)), dma((n_u, n_u, 2)),
            dma((n_u,)), dma((n_u,)),
        ]
    else:
        body = kernel
        scratch = buffers + [
            pltpu.VMEM((heads, 2 * n_u, rows // 2, head), BF), keys,
            attended, mixed, mixed,
        ] + line_sems + block_sems + [
            dma((n_u, n_u)), dma((n_u, n_u)), dma((n_u, n_u)),
            dma((n_u,)), dma((n_u,)),
        ]
    return pl.pallas_call(
        functools.partial(body, n_u, n_blk),
        out_shape=jax.ShapeDtypeStruct((rows, model), BF),
        in_specs=[early, early, early, early, hbm, vmem, vmem, hbm],
        out_specs=vmem,
        scratch_shapes=scratch,
        compiler_params=pltpu.CompilerParams(
            collective_id=0, has_side_effects=True, vmem_limit_bytes=66_000_000
        ),
    )(
        tokens, mod_shift[None], mod_scale[None], mod_gate[None],
        qkv_weight, query_gain[None], key_gain[None], out_weight,
    )


def solution(mesh):
    in_specs = (
        P(("blk", "ulysses"), None), P(), P(), P(),
        P(None, None, "ulysses"), P(), P(), P(None, "ulysses"),
    )
    out_specs = P(("blk", "ulysses"), None)
    body = functools.partial(local, mesh.shape["ulysses"], mesh.shape["blk"])
    return jax.shard_map(body, mesh=mesh, in_specs=in_specs, out_specs=out_specs, check_vma=False)
```

```python
import functools
import math

import jax
import jax.numpy as jnp
from jax import lax
from jax.experimental import pallas as pl
from jax.experimental.pallas import tpu as pltpu
from jax.sharding import PartitionSpec as P

MESH = pl.DeviceIdType.MESH
BF = jnp.bfloat16
F32 = jnp.float32
SPLIT = 2


def highest_bit(mask):
    return 1 << (mask.bit_length() - 1)


def lowest_bit(mask):
    return mask & -mask


def source_slot(mask, part):
    if mask & 1:
        return mask - 1, 1
    bit = highest_bit(mask) if part == 0 else lowest_bit(mask)
    return mask - bit, bit


def kernel(
    n_u, n_blk,
    tok_ref, shift_ref, scale_ref, gate_ref, w_hbm, qg_ref, kg_ref, wo_hbm, out_ref,
    w_ref, wo_ref, mod, q_ref, kv, att, stage, br,
    w_sem, sa_r, sa_l, ra, sb, rb, sc_r, sc_l, rc, sd, rd,
):
    z = lax.axis_index("ulysses")
    b = lax.axis_index("blk")
    rows, model = tok_ref.shape
    head = qg_ref.shape[1]
    width = w_ref.shape[2]
    heads = width // head
    factor = 1.0 / math.sqrt(head)
    last = n_u - 1
    half = rows // 2
    bits = [1 << i for i in range(n_blk.bit_length() - 1)]
    pair = 2 if heads % 2 == 0 else heads
    tile = pair * head

    for j in (1, 2, 0):
        pltpu.make_async_copy(w_hbm.at[j], w_ref.at[j], w_sem.at[j]).start()
    pltpu.make_async_copy(wo_hbm, wo_ref, w_sem.at[3]).start()

    def flip(bit):
        return b + (1 - 2 * ((b // bit) % 2)) * bit

    barrier = pltpu.get_barrier_semaphore()
    for d in range(1, n_u):
        pl.semaphore_signal(
            barrier, inc=1, device_id={"ulysses": (z + d) % n_u}, device_id_type=MESH
        )
    for bit in bits:
        pl.semaphore_signal(barrier, inc=1, device_id={"blk": flip(bit)}, device_id_type=MESH)

    wide = tok_ref[...].astype(F32)
    center = jnp.mean(wide, axis=-1, keepdims=True)
    spread = jnp.mean((wide - center) ** 2, axis=-1, keepdims=True)
    normed = (wide - center) * lax.rsqrt(spread + 1e-06)
    modulated = (normed * (1.0 + scale_ref[...]) + shift_ref[...]).astype(BF)
    mod[pl.ds(2 * z, 2)] = modulated.reshape(2, half, model)

    pl.semaphore_wait(barrier, n_u - 1 + len(bits))

    def line_copy(buf, index, send, recv, step):
        return pltpu.make_async_remote_copy(
            src_ref=buf.at[index], dst_ref=buf.at[index],
            send_sem=send.at[index], recv_sem=recv.at[index],
            device_id={"ulysses": z + step}, device_id_type=MESH,
        )

    def a_right(o):
        return line_copy(mod, o, sa_r, ra, 1)

    def a_left(o):
        return line_copy(mod, o, sa_l, ra, -1)

    def b_copy(mask, part, s):
        slot, bit = source_slot(mask, part)
        return pltpu.make_async_remote_copy(
            src_ref=kv.at[part, :, slot, s], dst_ref=kv.at[part, :, mask, s],
            send_sem=sb.at[mask, part, s], recv_sem=rb.at[mask, part, s],
            device_id={"blk": flip(bit)}, device_id_type=MESH,
        )

    masks = range(1, n_blk)

    def b_send(slot, part, s):
        for mask in sorted(masks, key=lambda m: m & 1):
            if source_slot(mask, part)[0] == slot:
                b_copy(mask, part, s).start()

    def b_level(level, s):
        for part in (0, 1):
            for mask in masks:
                if mask % 2 == 0 and bin(mask).count("1") == level:
                    b_copy(mask, part, s).wait_recv()
                    b_send(mask, part, s)

    levels = range(1, len(bits))

    def head_norm(sums, gain, scale):
        meansq = jnp.mean(sums * sums, axis=-1, keepdims=True)
        return sums * lax.rsqrt(meansq + 1e-06) * gain * scale

    def project(j, first, count, put):
        def body(i, _):
            start = pl.multiple_of(i * tile, tile)
            sums = jnp.dot(
                mod[pl.ds(first, count)].reshape(count * half, model),
                w_ref[j, :, pl.ds(start, tile)],
                preferred_element_type=F32,
            )
            for e in range(pair):
                put(i * pair + e, sums[:, e * head:(e + 1) * head])
            return 0

        lax.fori_loop(0, heads // pair, body, 0)

    def project_chunk(first, count, own=False):
        units = pl.ds(first, count)

        def ready(j):
            if own:
                pltpu.make_async_copy(w_hbm.at[j], w_ref.at[j], w_sem.at[j]).wait()

        def put_key(h, sums):
            keys = head_norm(sums, kg_ref[...], 1.0).astype(BF)
            kv[0, h, 0, units] = keys.reshape(count, half, head)

        def put_value(h, sums):
            kv[1, h, 0, units] = sums.astype(BF).reshape(count, half, head)

        def put_query(h, sums):
            queries = head_norm(sums, qg_ref[...], factor).astype(BF)
            q_ref[h, units] = queries.reshape(count, half, head)

        ready(1)
        project(1, first, count, put_key)
        for u in range(count):
            b_send(0, 0, first + u)
        ready(2)
        project(2, first, count, put_value)
        for u in range(count):
            b_send(0, 1, first + u)
        ready(0)
        project(0, first, count, put_query)

    for u in range(2):
        @pl.when(z < last)
        def _():
            a_right(2 * z + u).start()

        @pl.when(z > 0)
        def _():
            a_left(2 * z + u).start()

    project_chunk(2 * z, 2, own=True)

    def at_distance(k, act):
        for side in (-1, 1):
            o = z + side * k

            @pl.when((o >= 0) & (o <= last))
            def _():
                act(o)

    def pass_levels(which):
        def act(o):
            for level in which:
                for u in range(2):
                    b_level(level, 2 * o + u)
        return act

    def receive(k):
        for u in range(2):
            @pl.when(z - k >= 0)
            def _():
                a_right(2 * (z - k) + u).wait_recv()

                @pl.when(z < last)
                def _():
                    a_right(2 * (z - k) + u).start()

            @pl.when(z + k <= last)
            def _():
                a_left(2 * (z + k) + u).wait_recv()

                @pl.when(z > 0)
                def _():
                    a_left(2 * (z + k) + u).start()

    def previous(k, which):
        if isinstance(k, int) and k == 1:
            pass_levels(which)(z)
        else:
            at_distance(k - 1, pass_levels(which))

    for k in range(1, last):
        receive(k)
        previous(k, levels[:1])
        at_distance(k, lambda o: project_chunk(2 * o, 2))
        previous(k, levels[1:])

    ends = (z == 0) | (z == last)
    far = last - z

    def far_half(u):
        @pl.when(ends)
        def _():
            @pl.when(z == 0)
            def _():
                a_left(2 * far + u).wait_recv()

            @pl.when(z > 0)
            def _():
                a_right(2 * far + u).wait_recv()

            project_chunk(2 * far + u, 1)

    def far_levels(u, which):
        @pl.when(ends)
        def _():
            for level in which:
                b_level(level, 2 * far + u)

    previous(last, levels[:1])
    far_half(0)
    previous(last, levels[1:])
    far_levels(0, levels[:1])
    far_half(1)
    far_levels(0, levels[1:])
    far_levels(1, levels)

    def b_finish(s, _):
        for part in (0, 1):
            for mask in masks:
                if mask % 2 == 1:
                    b_copy(mask, part, s).wait_recv()
        return 0

    lax.fori_loop(0, 2 * n_u, b_finish, 0)
    pltpu.make_async_copy(wo_hbm, wo_ref, w_sem.at[3]).wait()

    keys_all = n_blk * n_u * rows

    def order(i):
        return jnp.where(i % 2 == 0, i // 2, last - i // 2)

    def c_right(o, src):
        return pltpu.make_async_remote_copy(
            src_ref=att.at[o, src], dst_ref=att.at[o, src],
            send_sem=sc_r.at[o, src], recv_sem=rc.at[o, src],
            device_id={"ulysses": z + 1}, device_id_type=MESH,
        )

    def c_left(o, src):
        return pltpu.make_async_remote_copy(
            src_ref=att.at[o, src], dst_ref=att.at[o, src],
            send_sem=sc_l.at[o, src], recv_sem=rc.at[o, src],
            device_id={"ulysses": z - 1}, device_id_type=MESH,
        )

    def d_copy(o, src):
        return pltpu.make_async_remote_copy(
            src_ref=stage.at[o], dst_ref=br.at[src],
            send_sem=sd.at[o], recv_sem=rd.at[src],
            device_id={"ulysses": o}, device_id_type=MESH,
        )

    group = 2 if n_u % 2 == 0 else 1

    def attend(chunks):
        for h in range(heads):
            keys = kv[0, h].reshape(keys_all, head)
            values = kv[1, h].reshape(keys_all, head)
            queries = jnp.concatenate(
                [q_ref[h, pl.ds(2 * o, 2)].reshape(rows, head) for o in chunks], axis=0
            )
            scores = lax.dot_general(
                queries, keys, (((1,), (1,)), ((), ())), preferred_element_type=F32
            )
            powers = jnp.exp(scores - jnp.max(scores, axis=-1, keepdims=True))
            total = jnp.sum(powers, axis=-1, keepdims=True)
            numerator = jnp.dot(powers.astype(BF), values, preferred_element_type=F32)
            result = (numerator / total).astype(BF)
            for g, o in enumerate(chunks):
                att[o, z, :, h * head:(h + 1) * head] = result[g * rows:(g + 1) * rows]

    def pass_right(o, src):
        c_right(o, src).wait_recv()

        @pl.when(z < last)
        def _():
            c_right(o, src).start()

    def pass_left(o, src):
        c_left(o, src).wait_recv()

        @pl.when(z > 0)
        def _():
            c_left(o, src).start()

    low = z < n_u // 2

    def attend_step(t, _):
        @pl.when(t < n_u // group)
        def _():
            chunks = [order(group * t + g) for g in range(group)]
            attend(chunks)
            for o in chunks:
                @pl.when(z < last)
                def _():
                    c_right(o, z).start()

                @pl.when(z > 0)
                def _():
                    c_left(o, z).start()

        for g in range(group):
            @pl.when((t > 0) & low & (z > 0))
            def _():
                pass_left(order(group * (t - 1) + g), z + 1)

            @pl.when((t > 0) & jnp.logical_not(low) & (z < last))
            def _():
                pass_right(order(group * (t - 1) + g), z - 1)

        return 0

    lax.fori_loop(0, n_u // group + 1, attend_step, 0)

    def mix_step(t, _):
        for k in range(last, 0, -1):
            i = t - k + 1
            held = (i >= 0) & (i < n_u)
            right_too = held & (z - k >= 0)
            left_too = held & (z + k <= last)
            if k == 1:
                right_too = right_too & (low | (z == last))
                left_too = left_too & (jnp.logical_not(low) | (z == 0))

            @pl.when(right_too)
            def _():
                pass_right(order(i), z - k)

            @pl.when(left_too)
            def _():
                pass_left(order(i), z + k)

        @pl.when(t >= last - 1)
        def _():
            o = order(t - last + 1)
            total = jnp.zeros((rows, width), F32)
            for src in range(n_u):
                total += jnp.dot(
                    att[o, src], wo_ref[src * width:(src + 1) * width, :],
                    preferred_element_type=F32,
                )

            @pl.when(o == z)
            def _():
                br[z] = total.astype(BF)

            @pl.when(o != z)
            def _():
                stage[o] = total.astype(BF)
                d_copy(o, z).start()

        return 0

    lax.fori_loop(0, n_u + last - 1, mix_step, 0)

    for src in range(n_u):
        @pl.when(src != z)
        def _():
            d_copy(src, src).wait_recv()

        cols = slice(src * width, (src + 1) * width)
        out_ref[:, cols] = (
            tok_ref[:, cols].astype(F32) + gate_ref[:, cols] * br[src].astype(F32)
        ).astype(BF)

    def finish(s, _):
        for u in range(2):
            @pl.when((s <= z) & (z < last))
            def _():
                a_right(2 * s + u).wait_send()

            @pl.when((s >= z) & (z > 0))
            def _():
                a_left(2 * s + u).wait_send()

        for src in range(n_u):
            @pl.when((src <= z) & (z < last))
            def _():
                c_right(s, src).wait_send()

            @pl.when((src >= z) & (z > 0))
            def _():
                c_left(s, src).wait_send()

        @pl.when(s != z)
        def _():
            d_copy(s, z).wait_send()

        for part in (0, 1):
            for mask in masks:
                for u in range(2):
                    b_copy(mask, part, 2 * s + u).wait_send()
        return 0

    lax.fori_loop(0, n_u, finish, 0)


def split_kernel(
    n_u, n_blk,
    tok_hbm, shift_hbm, scale_hbm, gate_hbm, w_hbm, qg_ref, kg_ref, wo_hbm, out_ref,
    w_ref, wo_ref, mod, q_ref, kv, wx_ref, att, xatt, pair_ref, stage, br,
    tok_ref, shift_ref, scale_ref, gate_ref, in_sem, swz, rwz, sw, rw, rw_core,
    w_sem, sa_r, sa_l, ra, sb, rb, rb_core, sq, rq, sx, rx, sc, rc, sd, rd,
):
    z = lax.axis_index("ulysses")
    b = lax.axis_index("blk")
    rows, model = tok_ref.shape
    head = qg_ref.shape[1]
    width = w_ref.shape[2]
    heads = width // head
    share = heads // 2
    cols = share * head
    factor = 1.0 / math.sqrt(head)
    last = n_u - 1
    half = rows // 2
    bits = [1 << i for i in range(n_blk.bit_length() - 1)]
    masks = range(1, n_blk)
    side = (b // SPLIT) % 2
    mine = side * share
    theirs = (1 - side) * share
    line_half = n_u // 2
    low = z < line_half
    hub = jnp.where(low, line_half - 1, line_half)
    is_hub = z == hub
    onward = jnp.where(low, 1, -1)
    away = jnp.where(low, hub - z, z - hub)
    slice_rows = model // n_blk
    part_rows = slice_rows // 2

    def flip(bit):
        return b + (1 - 2 * ((b // bit) % 2)) * bit

    barrier = pltpu.get_barrier_semaphore()
    for d in range(1, n_u):
        pl.semaphore_signal(
            barrier, inc=1, device_id={"ulysses": (z + d) % n_u}, device_id_type=MESH
        )
    for bit in bits:
        pl.semaphore_signal(barrier, inc=1, device_id={"blk": flip(bit)}, device_id_type=MESH)

    inputs = [
        pltpu.make_async_copy(src, dst, in_sem.at[i])
        for i, (src, dst) in enumerate((
            (tok_hbm, tok_ref), (shift_hbm, shift_ref), (scale_hbm, scale_ref), (gate_hbm, gate_ref),
        ))
    ]
    for copy in inputs:
        copy.start()
    for copy in inputs:
        copy.wait()
    own_slice = pl.ds(pl.multiple_of(b * slice_rows, 16), slice_rows)
    wo_slice = pltpu.make_async_copy(wo_hbm.at[own_slice], wo_ref.at[own_slice], w_sem.at[3])
    wo_whole = pltpu.make_async_copy(wo_hbm, wo_ref, w_sem.at[3])

    @pl.when(jnp.logical_not(is_hub))
    def _():
        wo_slice.start()

    for j in (1, 2, 0):
        pltpu.make_async_copy(w_hbm.at[j], w_ref.at[j], w_sem.at[j]).start()

    @pl.when(is_hub)
    def _():
        wo_whole.start()


    wide = tok_ref[...].astype(F32)
    center = jnp.mean(wide, axis=-1, keepdims=True)
    spread = jnp.mean((wide - center) ** 2, axis=-1, keepdims=True)
    normed = (wide - center) * lax.rsqrt(spread + 1e-06)
    modulated = (normed * (1.0 + scale_ref[...]) + shift_ref[...]).astype(BF)
    mod[pl.ds(2 * z, 2)] = modulated.reshape(2, half, model)

    with jax.named_scope("barrier"):
        pl.semaphore_wait(barrier, n_u - 1 + len(bits))

    def line_copy(buf, index, send, recv, step):
        return pltpu.make_async_remote_copy(
            src_ref=buf.at[index], dst_ref=buf.at[index],
            send_sem=send.at[index], recv_sem=recv.at[index],
            device_id={"ulysses": z + step}, device_id_type=MESH,
        )

    def a_right(o):
        return line_copy(mod, o, sa_r, ra, 1)

    def a_left(o):
        return line_copy(mod, o, sa_l, ra, -1)

    def drain(ref, sem):
        pltpu.make_async_copy(ref, ref, sem).wait()

    def rows_of(origin, part):
        return pl.ds(pl.multiple_of(origin * slice_rows + part * part_rows, 16), part_rows)

    def origin_of(mask):
        return b + sum((1 - 2 * ((b // bit) % 2)) * bit for bit in bits if mask & bit)

    def wz_copy(part, slot):
        return pltpu.make_async_remote_copy(
            src_ref=wo_ref.at[rows_of(b, part)], dst_ref=wx_ref.at[slot, rows_of(b, part)],
            send_sem=swz.at[part], recv_sem=rwz.at[slot, part],
            device_id={"ulysses": hub}, device_id_type=MESH,
        )

    def w_copy(mask, part):
        slot, bit = source_slot(mask, part)
        ref = wx_ref.at[:, rows_of(origin_of(slot), part)]
        return pltpu.make_async_remote_copy(
            src_ref=ref, dst_ref=ref,
            send_sem=sw, recv_sem=rw_core if mask & 1 else rw.at[mask // 2, part],
            device_id={"blk": flip(bit)}, device_id_type=MESH,
        )

    def w_wait(mask, part):
        ref = wx_ref.at[:, rows_of(origin_of(mask), part)]
        pltpu.make_async_remote_copy(
            src_ref=ref, dst_ref=ref,
            send_sem=sw, recv_sem=rw.at[mask // 2, part],
            device_id={"blk": flip(source_slot(mask, part)[1])}, device_id_type=MESH,
        ).wait_recv()

    def w_relay(mask, part):
        w_wait(mask, part)
        for later in sorted(masks, key=lambda m: m & 1):
            if source_slot(later, part)[0] == mask:
                w_copy(later, part).start()

    def source(mask, part):
        if mask & 1:
            return mask - 1, 1
        if mask == SPLIT:
            return 0, SPLIT
        rest = mask & ~SPLIT
        bit = highest_bit(rest) if part == 0 else lowest_bit(rest)
        return mask - bit, bit

    def b_sem(mask, part, u):
        return rb_core if mask & 1 else rb.at[mask // 2, part, u]

    def b_copy(mask, part, u):
        slot, bit = source(mask, part)
        own = pl.ds(theirs if bit == SPLIT else mine, share)
        return pltpu.make_async_remote_copy(
            src_ref=kv.at[part, own, slot, u], dst_ref=kv.at[part, own, mask, u],
            send_sem=sb, recv_sem=b_sem(mask, part, u),
            device_id={"blk": flip(bit)}, device_id_type=MESH,
        )

    def b_cross(bit, part, u):
        own = pl.ds(theirs, share)
        return pltpu.make_async_remote_copy(
            src_ref=kv.at[part, own, 0, u], dst_ref=kv.at[part, own, SPLIT + bit, u],
            send_sem=sb, recv_sem=b_sem(SPLIT + bit, part, u),
            device_id={"blk": origin_of(SPLIT + bit)}, device_id_type=MESH,
        )

    def b_wait(mask, part, u):
        here = kv.at[part, pl.ds(mine, share), mask, u]
        pltpu.make_async_remote_copy(
            src_ref=here, dst_ref=here,
            send_sem=sb, recv_sem=b_sem(mask, part, u),
            device_id={"blk": flip(source(mask, part)[1])}, device_id_type=MESH,
        ).wait_recv()

    def q_copy(u, first):
        heads_of = pl.ds(first, share)
        return pltpu.make_async_remote_copy(
            src_ref=q_ref.at[heads_of, 0, u], dst_ref=q_ref.at[heads_of, 1, u],
            send_sem=sq, recv_sem=rq,
            device_id={"blk": flip(SPLIT)}, device_id_type=MESH,
        )

    def b_send(slot, part, u, cross=False):
        for mask in sorted(masks, key=lambda m: (m & 1, m != SPLIT)):
            at, bit = source(mask, part)
            if at == slot and not (cross and slot == SPLIT and bit != 1):
                b_copy(mask, part, u).start()
                if cross and mask == SPLIT:
                    for far_bit in bits[2:]:
                        b_cross(far_bit, part, u).start()

    def depth_of(mask):
        return bin(mask).count("1")

    def b_level(level, u, cross=False):
        for part in (0, 1):
            for mask in masks:
                if mask % 2 == 0 and depth_of(mask) == level:
                    b_wait(mask, part, u)
                    b_send(mask, part, u, cross)

    depth = len(bits) - 1

    def level_one(o):
        for u in range(2):
            b_level(1, 2 * o + u)

    def level_rest(o):
        for level in range(2, depth + 1):
            for u in range(2):
                b_level(level, 2 * o + u)

    def head_norm(sums, gain, scale):
        meansq = jnp.mean(sums * sums, axis=-1, keepdims=True)
        return sums * lax.rsqrt(meansq + 1e-06) * gain * scale

    def project(starts, count, own=False, between=None, cross=False):
        size = count * half

        def sums_of(j):
            if own:
                pltpu.make_async_copy(w_hbm.at[j], w_ref.at[j], w_sem.at[j]).wait()
            tokens = [mod[pl.ds(first, count)].reshape(size, model) for first in starts]
            sums = jnp.dot(
                jnp.concatenate(tokens, axis=0), w_ref[j], preferred_element_type=F32
            )
            return [sums[:, h * head:(h + 1) * head] for h in range(heads)]

        def put(value, at):
            for i, first in enumerate(starts):
                at(pl.ds(first, count), value[i * size:(i + 1) * size].reshape(count, half, head))

        def send(act):
            for first in starts:
                for u in range(count):
                    act(first + u)

        for h, sums in enumerate(sums_of(1)):
            def put_keys(units, part):
                kv[0, h, 0, units] = part
            put(head_norm(sums, kg_ref[...], 1.0).astype(BF), put_keys)
        send(lambda u: b_send(0, 0, u, cross))
        for h, sums in enumerate(sums_of(2)):
            def put_values(units, part):
                kv[1, h, 0, units] = part
            put(sums.astype(BF), put_values)
        send(lambda u: b_send(0, 1, u, cross))
        if between is not None:
            between()
        for h, sums in enumerate(sums_of(0)):
            def put_queries(units, part):
                q_ref[h, 0, units] = part
            put(head_norm(sums, qg_ref[...], factor).astype(BF), put_queries)
        send(lambda u: q_copy(u, theirs).start())

    for u in range(2):
        @pl.when(z < last)
        def _():
            a_right(2 * z + u).start()

        @pl.when(z > 0)
        def _():
            a_left(2 * z + u).start()

    @pl.when(jnp.logical_not(is_hub))
    def _():
        wo_slice.wait()
        for part in range(2):
            wz_copy(part, away - 1).start()

    def receive(k, u):
        @pl.when(z - k >= 0)
        def _():
            a_right(2 * (z - k) + u).wait_recv()

            @pl.when(z < last)
            def _():
                a_right(2 * (z - k) + u).start()

        @pl.when(z + k <= last)
        def _():
            a_left(2 * (z + k) + u).wait_recv()

            @pl.when(z > 0)
            def _():
                a_left(2 * (z + k) + u).start()

    def at_each(k, act):
        @pl.when(z >= k)
        def _():
            act(z - k)

        @pl.when((z + k <= last) & (k > 0))
        def _():
            act(z + k)

    def project_at(k, between):
        two = (z >= k) & (z + k <= last)

        @pl.when(two)
        def _():
            project([2 * (z - k), 2 * (z + k)], 2, between=between)

        @pl.when(jnp.logical_not(two) & ((z >= k) | (z + k <= last)))
        def _():
            project([2 * jnp.where(z >= k, z - k, z + k)], 2, between=between)

    with jax.named_scope("own"):
        project([2 * z], 2, own=True)
    receive(1, 0)
    level_one(z)
    if last > 1:
        receive(1, 1)

    def line_step(k, _):
        def between():
            @pl.when(k + 1 < last)
            def _():
                at_each(k - 1, level_rest)

        with jax.named_scope("project"):
            project_at(k, between)
        receive(k + 1, 0)

        @pl.when(k + 1 < last)
        def _():
            at_each(k, level_one)
            receive(k + 1, 1)

        return 0

    with jax.named_scope("line"):
        lax.fori_loop(1, last, line_step, 0)

    ends = (z == 0) | (z == last)
    far = last - z

    first_part = [(SPLIT, 0), (1, 0), (1, 1)]
    direct = [
        (mask, part) for part in (1, 0) for mask in masks
        if mask % 2 == 0 and mask != SPLIT and source_slot(mask, part)[0] == 0
    ]

    @pl.when(is_hub)
    def _():
        for part in range(2):
            for slot in range(line_half - 1):
                wz_copy(part, slot).wait_recv()
        for mask, part in first_part:
            w_copy(mask, part).start()

    with jax.named_scope("far"):
        @pl.when(jnp.logical_not(ends))
        def _():
            at_each(last - 1, level_one)
            at_each(last - 2, level_rest)
            at_each(last - 1, level_rest)

        def far_step(u, _):
            @pl.when(u == 1)
            def _():
                receive(last, 1)

            def between():
                @pl.when(u == 0)
                def _():
                    at_each(last - 1, level_one)

            with jax.named_scope("project_half"):
                project([2 * far + u], 1, between=between, cross=True)
            return 0

        @pl.when(ends)
        def _():
            lax.fori_loop(0, 2, far_step, 0)
            at_each(last - 2, level_rest)
            b_level(1, 2 * far, cross=True)
            at_each(last - 1, level_rest)
            b_level(1, 2 * far + 1, cross=True)
            for level in range(2, depth + 1):
                b_level(level, 2 * far, cross=True)
                b_level(level, 2 * far + 1, cross=True)

    @pl.when(is_hub)
    def _():
        for mask, part in direct:
            w_copy(mask, part).start()

    with jax.named_scope("b_finish"):
        drain(kv.at[:, pl.ds(0, share), pl.ds(0, n_blk // 2)], rb_core)
        drain(q_ref.at[pl.ds(0, share), 0], rq)

    keys_all = n_blk * n_u * rows

    def order(i, rightward):
        leftward = jnp.where(i < line_half, last - i, i - line_half)
        return jnp.where(rightward, last - leftward, leftward)

    def c_copy(o, src, sd):
        ref = att.at[o, src, :, pl.ds(pl.multiple_of(sd * cols, head), cols)]
        return pltpu.make_async_remote_copy(
            src_ref=ref, dst_ref=ref,
            send_sem=sc.at[src], recv_sem=rc.at[o, src, sd],
            device_id={"ulysses": z + onward}, device_id_type=MESH,
        )

    def c_send(t, sd):
        c_copy(order(t, low), z, sd).start()

    def x_copy(o, sd):
        return pltpu.make_async_remote_copy(
            src_ref=xatt.at[o],
            dst_ref=att.at[o, z, :, pl.ds(pl.multiple_of(sd * cols, head), cols)],
            send_sem=sx, recv_sem=rx.at[o],
            device_id={"blk": flip(SPLIT)}, device_id_type=MESH,
        )

    def quarter(d):
        return hub - onward * d

    def d_copy(o, d):
        return pltpu.make_async_remote_copy(
            src_ref=stage.at[o, d], dst_ref=br.at[quarter(d)],
            send_sem=sd, recv_sem=rd.at[quarter(d)],
            device_id={"ulysses": o}, device_id_type=MESH,
        )

    def attend(t):
        first, second = t == 0, t == n_u - 1
        groups = (
            (first, order(jnp.where(first, 0, t - 1), low)),
            (jnp.logical_not(second), order(jnp.where(second, t, t + 1), low)),
        )
        for r in range(share):
            h = mine + r
            keys = kv[0, h].reshape(keys_all, head)
            values = kv[1, h].reshape(keys_all, head)
            queries = jnp.concatenate([
                q_ref[h, jnp.where(away, 1, 0), pl.ds(2 * o, 2)].reshape(rows, head)
                for away, o in groups
            ], axis=0)
            scores = lax.dot_general(
                queries, keys, (((1,), (1,)), ((), ())), preferred_element_type=F32
            )
            powers = jnp.exp(scores - jnp.max(scores, axis=-1, keepdims=True))
            total = jnp.sum(powers, axis=-1, keepdims=True)
            numerator = jnp.dot(powers.astype(BF), values, preferred_element_type=F32)
            pair_ref[:, r * head:(r + 1) * head] = (numerator / total).astype(BF)
        for g, (away, o) in enumerate(groups):
            @pl.when(away)
            def _():
                xatt[o] = pair_ref[g * rows:(g + 1) * rows]
                x_copy(o, side).start()

            @pl.when(jnp.logical_not(away))
            def _():
                place = pl.ds(pl.multiple_of(side * cols, head), cols)
                att[o, z, :, place] = pair_ref[g * rows:(g + 1) * rows]

        @pl.when(t > 0)
        def _():
            c_send(t - 1, side)

        @pl.when(second)
        def _():
            c_send(t, side)

    def pass_on(i, k):
        src = z - onward * k
        there = (src >= 0) & (src <= last)

        @pl.when(there & (i >= 0) & (i < n_u))
        def _():
            copy = c_copy(order(i, low), src, side)
            copy.wait_recv()
            copy.start()

        @pl.when(there & (i >= 1) & (i <= n_u))
        def _():
            copy = c_copy(order(i - 1, low), src, 1 - side)
            copy.wait_recv()
            copy.start()

    def x_step(t):
        x_copy(order(t, low), 1 - side).wait_recv()
        c_send(t, 1 - side)

    def attend_step(t, _):
        with jax.named_scope("attend"):
            attend(t)

        @pl.when(is_hub & (t == n_u - 2))
        def _():
            w_copy(SPLIT, 1).start()

        @pl.when(t > 1)
        def _():
            x_step(t - 2)

        return 0

    with jax.named_scope("attend_loop"):
        lax.fori_loop(0, n_u, attend_step, 0)

        for t in range(max(n_u - 2, 0), n_u):
            x_step(t)

        @pl.when(is_hub)
        def _():
            w_relay(SPLIT, 0)
            w_relay(2 * SPLIT, 1)

    def mix(indices, weights, d):
        chunks = [order(i, jnp.logical_not(low)) for i in indices]
        with jax.named_scope("mix"):
            total = jnp.zeros((len(chunks) * rows, width), F32)
            for src in range(n_u):
                total += jnp.dot(
                    jnp.concatenate([att[o, src] for o in chunks], axis=0),
                    weights[src * width:(src + 1) * width, :],
                    preferred_element_type=F32,
                )
            result = total.astype(BF)
        for g, o in enumerate(chunks):
            part = result[g * rows:(g + 1) * rows]

            @pl.when(o == z)
            def _():
                br[quarter(d)] = part

            @pl.when(o != z)
            def _():
                stage[o, d] = part
                d_copy(o, d).start()

    def gathered(i):
        for k in range(line_half):
            for sd_of in (side, 1 - side):
                c_copy(order(i, jnp.logical_not(low)), hub + onward * (k + 1), sd_of).wait_recv()

    gap = 2
    steps = n_u + 1 + gap * (line_half - 2)

    def pass_step(t, _):
        for k in range(1, line_half):
            pass_on(t - gap * (k - 1), k)

        @pl.when(is_hub & (t == 1))
        def _():
            w_relay(SPLIT, 1)
            w_relay(2 * SPLIT, 0)

        i = t - (steps - line_half)

        @pl.when(is_hub & (i >= 0))
        def _():
            gathered(i)
            mix([i], wo_ref, 0)

        return 0

    with jax.named_scope("pass_loop"):
        @pl.when(is_hub)
        def _():
            wo_whole.wait()

        lax.fori_loop(0, steps, pass_step, 0)

    with jax.named_scope("hub"):
        @pl.when(is_hub)
        def _():
            with jax.named_scope("w_last"):
                for mask in sorted(masks, key=depth_of):
                    if mask % 2 == 0 and mask not in (SPLIT, 2 * SPLIT):
                        for part in range(2):
                            w_relay(mask, part)
                drain(wx_ref.at[:, pl.ds(0, n_blk // 2 * slice_rows)], rw_core)

            first, second = range(line_half), range(line_half, n_u)
            for d in range(1, line_half):
                mix(first, wx_ref.at[d - 1], d)
            for group in ([i for i in second[:-1]], [n_u - 1]):
                for i in group:
                    gathered(i)
                mix(group, wo_ref, 0)
                for d in range(1, line_half):
                    mix(group, wx_ref.at[d - 1], d)

    with jax.named_scope("final"):
        for src in range(n_u):
            @pl.when(jnp.logical_not(is_hub) | (low != (src < line_half)))
            def _():
                pltpu.make_async_remote_copy(
                    src_ref=br.at[src], dst_ref=br.at[src],
                    send_sem=rd.at[src], recv_sem=rd.at[src],
                    device_id={"ulysses": last - hub}, device_id_type=MESH,
                ).wait_recv()

            at = slice(src * width, (src + 1) * width)
            out_ref[:, at] = (
                tok_ref[:, at].astype(F32) + gate_ref[:, at] * br[src].astype(F32)
            ).astype(BF)

    def finish(s, _):
        for u in range(2):
            @pl.when((s <= z) & (z < last))
            def _():
                a_right(2 * s + u).wait_send()

            @pl.when((s >= z) & (z > 0))
            def _():
                a_left(2 * s + u).wait_send()

        @pl.when(jnp.where(low, s <= z, s >= z))
        def _():
            drain(att.at[:, s], sc.at[s])

        return 0

    with jax.named_scope("finish"):
        lax.fori_loop(0, n_u, finish, 0)

        drain(xatt, sx)
        drain(q_ref.at[pl.ds(0, share), 0], sq)
        drain(kv.at[:, pl.ds(0, share), pl.ds(1, n_blk - 1)], sb)

        @pl.when(is_hub)
        def _():
            drain(stage.at[pl.ds(0, n_u - 1)], sd)
            drain(wx_ref.at[:, pl.ds(0, (n_blk - 1) * slice_rows)], sw)

        @pl.when(jnp.logical_not(is_hub))
        def _():
            for part in range(2):
                wz_copy(part, away - 1).wait_send()


def local(n_u, n_blk, tokens, mod_shift, mod_scale, mod_gate, qkv_weight, query_gain, key_gain, out_weight):
    rows, model = tokens.shape
    width = qkv_weight.shape[2]
    head = query_gain.shape[0]
    heads = width // head
    vmem = pl.BlockSpec(memory_space=pltpu.VMEM)
    hbm = pl.BlockSpec(memory_space=pltpu.HBM)
    dma = pltpu.SemaphoreType.DMA
    split = heads % 2 == 0 and n_blk % (2 * SPLIT) == 0 and n_u % 2 == 0 and n_u > 2
    buffers = [
        pltpu.VMEM(qkv_weight.shape, BF),
        pltpu.VMEM(out_weight.shape, BF),
        pltpu.VMEM((2 * n_u, rows // 2, model), BF),
    ]
    line_sems = [dma((4,)), dma((2 * n_u,)), dma((2 * n_u,)), dma((2 * n_u,))]
    block_sems = [dma((n_blk, 2, 2 * n_u)), dma((n_blk, 2, 2 * n_u))]
    keys = pltpu.VMEM((2, heads, n_blk, 2 * n_u, rows // 2, head), BF)
    attended = pltpu.VMEM((n_u, n_u, rows, width), BF)
    mixed = pltpu.VMEM((n_u, rows, width), BF)
    row = pltpu.VMEM((1, model), F32)
    early = hbm if split else vmem
    one = pltpu.SemaphoreType.DMA
    if split:
        body = split_kernel
        scratch = buffers + [
            pltpu.VMEM((heads, 2, 2 * n_u, rows // 2, head), BF), keys,
            pltpu.VMEM((n_u // 2 - 1, *out_weight.shape), BF),
            attended, pltpu.VMEM((n_u, rows, width // 2), BF),
            pltpu.VMEM((2 * rows, width // 2), BF),
            pltpu.VMEM((n_u, n_u // 2, rows, width), BF), mixed,
            pltpu.VMEM((rows, model), BF), row, row, row, dma((4,)),
            dma((2,)), dma((n_u // 2 - 1, 2)), one, dma((n_blk // 2, 2)), one,
        ] + line_sems + [
            one, dma((n_blk // 2, 2, 2 * n_u)), one, one, one, one, dma((n_u,)),
            dma((n_u,)), dma((n_u, n_u, 2)), one, dma((n_u,)),
        ]
    else:
        body = kernel
        scratch = buffers + [
            pltpu.VMEM((heads, 2 * n_u, rows // 2, head), BF), keys,
            attended, mixed, mixed,
        ] + line_sems + block_sems + [
            dma((n_u, n_u)), dma((n_u, n_u)), dma((n_u, n_u)),
            dma((n_u,)), dma((n_u,)),
        ]
    return pl.pallas_call(
        functools.partial(body, n_u, n_blk),
        out_shape=pltpu.VMEM((rows, model), BF) if split else jax.ShapeDtypeStruct((rows, model), BF),
        in_specs=[early, early, early, early, hbm, vmem, vmem, hbm],
        out_specs=vmem,
        scratch_shapes=scratch,
        compiler_params=pltpu.CompilerParams(
            collective_id=0, has_side_effects=True, vmem_limit_bytes=63_000_000 if split else 66_000_000
        ),
    )(
        tokens, mod_shift[None], mod_scale[None], mod_gate[None],
        qkv_weight, query_gain[None], key_gain[None], out_weight,
    )


def solution(mesh):
    in_specs = (
        P(("blk", "ulysses"), None), P(), P(), P(),
        P(None, None, "ulysses"), P(), P(), P(None, "ulysses"),
    )
    out_specs = P(("blk", "ulysses"), None)
    body = functools.partial(local, mesh.shape["ulysses"], mesh.shape["blk"])
    return jax.shard_map(body, mesh=mesh, in_specs=in_specs, out_specs=out_specs, check_vma=False)
```

```python
import functools
import math

import jax
import jax.numpy as jnp
from jax import lax
from jax.experimental import pallas as pl
from jax.experimental.pallas import tpu as pltpu
from jax.sharding import PartitionSpec as P

MESH = pl.DeviceIdType.MESH
BF = jnp.bfloat16
F32 = jnp.float32
SPLIT = 2
Z_MASKS = (0, 3 * SPLIT)


def highest_bit(mask):
    return 1 << (mask.bit_length() - 1)


def lowest_bit(mask):
    return mask & -mask


def source_slot(mask, part):
    if mask & 1:
        return mask - 1, 1
    bit = highest_bit(mask) if part == 0 else lowest_bit(mask)
    return mask - bit, bit


def kernel(
    n_u, n_blk,
    tok_ref, shift_ref, scale_ref, gate_ref, w_hbm, qg_ref, kg_ref, wo_hbm, out_ref,
    w_ref, wo_ref, mod, q_ref, kv, att, stage, br,
    w_sem, sa_r, sa_l, ra, sb, rb, sc_r, sc_l, rc, sd, rd,
):
    z = lax.axis_index("ulysses")
    b = lax.axis_index("blk")
    rows, model = tok_ref.shape
    head = qg_ref.shape[1]
    width = w_ref.shape[2]
    heads = width // head
    factor = 1.0 / math.sqrt(head)
    last = n_u - 1
    half = rows // 2
    bits = [1 << i for i in range(n_blk.bit_length() - 1)]
    pair = 2 if heads % 2 == 0 else heads
    tile = pair * head

    for j in (1, 2, 0):
        pltpu.make_async_copy(w_hbm.at[j], w_ref.at[j], w_sem.at[j]).start()
    pltpu.make_async_copy(wo_hbm, wo_ref, w_sem.at[3]).start()

    def flip(bit):
        return b + (1 - 2 * ((b // bit) % 2)) * bit

    barrier = pltpu.get_barrier_semaphore()
    for d in range(1, n_u):
        pl.semaphore_signal(
            barrier, inc=1, device_id={"ulysses": (z + d) % n_u}, device_id_type=MESH
        )
    for bit in bits:
        pl.semaphore_signal(barrier, inc=1, device_id={"blk": flip(bit)}, device_id_type=MESH)

    wide = tok_ref[...].astype(F32)
    center = jnp.mean(wide, axis=-1, keepdims=True)
    spread = jnp.mean((wide - center) ** 2, axis=-1, keepdims=True)
    normed = (wide - center) * lax.rsqrt(spread + 1e-06)
    modulated = (normed * (1.0 + scale_ref[...]) + shift_ref[...]).astype(BF)
    mod[pl.ds(2 * z, 2)] = modulated.reshape(2, half, model)

    pl.semaphore_wait(barrier, n_u - 1 + len(bits))

    def line_copy(buf, index, send, recv, step):
        return pltpu.make_async_remote_copy(
            src_ref=buf.at[index], dst_ref=buf.at[index],
            send_sem=send.at[index], recv_sem=recv.at[index],
            device_id={"ulysses": z + step}, device_id_type=MESH,
        )

    def a_right(o):
        return line_copy(mod, o, sa_r, ra, 1)

    def a_left(o):
        return line_copy(mod, o, sa_l, ra, -1)

    def b_copy(mask, part, s):
        slot, bit = source_slot(mask, part)
        return pltpu.make_async_remote_copy(
            src_ref=kv.at[part, :, slot, s], dst_ref=kv.at[part, :, mask, s],
            send_sem=sb.at[mask, part, s], recv_sem=rb.at[mask, part, s],
            device_id={"blk": flip(bit)}, device_id_type=MESH,
        )

    masks = range(1, n_blk)

    def b_send(slot, part, s):
        for mask in sorted(masks, key=lambda m: m & 1):
            if source_slot(mask, part)[0] == slot:
                b_copy(mask, part, s).start()

    def b_level(level, s):
        for part in (0, 1):
            for mask in masks:
                if mask % 2 == 0 and bin(mask).count("1") == level:
                    b_copy(mask, part, s).wait_recv()
                    b_send(mask, part, s)

    levels = range(1, len(bits))

    def head_norm(sums, gain, scale):
        meansq = jnp.mean(sums * sums, axis=-1, keepdims=True)
        return sums * lax.rsqrt(meansq + 1e-06) * gain * scale

    def project(j, first, count, put):
        def body(i, _):
            start = pl.multiple_of(i * tile, tile)
            sums = jnp.dot(
                mod[pl.ds(first, count)].reshape(count * half, model),
                w_ref[j, :, pl.ds(start, tile)],
                preferred_element_type=F32,
            )
            for e in range(pair):
                put(i * pair + e, sums[:, e * head:(e + 1) * head])
            return 0

        lax.fori_loop(0, heads // pair, body, 0)

    def project_chunk(first, count, own=False):
        units = pl.ds(first, count)

        def ready(j):
            if own:
                pltpu.make_async_copy(w_hbm.at[j], w_ref.at[j], w_sem.at[j]).wait()

        def put_key(h, sums):
            keys = head_norm(sums, kg_ref[...], 1.0).astype(BF)
            kv[0, h, 0, units] = keys.reshape(count, half, head)

        def put_value(h, sums):
            kv[1, h, 0, units] = sums.astype(BF).reshape(count, half, head)

        def put_query(h, sums):
            queries = head_norm(sums, qg_ref[...], factor).astype(BF)
            q_ref[h, units] = queries.reshape(count, half, head)

        ready(1)
        project(1, first, count, put_key)
        for u in range(count):
            b_send(0, 0, first + u)
        ready(2)
        project(2, first, count, put_value)
        for u in range(count):
            b_send(0, 1, first + u)
        ready(0)
        project(0, first, count, put_query)

    for u in range(2):
        @pl.when(z < last)
        def _():
            a_right(2 * z + u).start()

        @pl.when(z > 0)
        def _():
            a_left(2 * z + u).start()

    project_chunk(2 * z, 2, own=True)

    def at_distance(k, act):
        for side in (-1, 1):
            o = z + side * k

            @pl.when((o >= 0) & (o <= last))
            def _():
                act(o)

    def pass_levels(which):
        def act(o):
            for level in which:
                for u in range(2):
                    b_level(level, 2 * o + u)
        return act

    def receive(k):
        for u in range(2):
            @pl.when(z - k >= 0)
            def _():
                a_right(2 * (z - k) + u).wait_recv()

                @pl.when(z < last)
                def _():
                    a_right(2 * (z - k) + u).start()

            @pl.when(z + k <= last)
            def _():
                a_left(2 * (z + k) + u).wait_recv()

                @pl.when(z > 0)
                def _():
                    a_left(2 * (z + k) + u).start()

    def previous(k, which):
        if isinstance(k, int) and k == 1:
            pass_levels(which)(z)
        else:
            at_distance(k - 1, pass_levels(which))

    for k in range(1, last):
        receive(k)
        previous(k, levels[:1])
        at_distance(k, lambda o: project_chunk(2 * o, 2))
        previous(k, levels[1:])

    ends = (z == 0) | (z == last)
    far = last - z

    def far_half(u):
        @pl.when(ends)
        def _():
            @pl.when(z == 0)
            def _():
                a_left(2 * far + u).wait_recv()

            @pl.when(z > 0)
            def _():
                a_right(2 * far + u).wait_recv()

            project_chunk(2 * far + u, 1)

    def far_levels(u, which):
        @pl.when(ends)
        def _():
            for level in which:
                b_level(level, 2 * far + u)

    previous(last, levels[:1])
    far_half(0)
    previous(last, levels[1:])
    far_levels(0, levels[:1])
    far_half(1)
    far_levels(0, levels[1:])
    far_levels(1, levels)

    def b_finish(s, _):
        for part in (0, 1):
            for mask in masks:
                if mask % 2 == 1:
                    b_copy(mask, part, s).wait_recv()
        return 0

    lax.fori_loop(0, 2 * n_u, b_finish, 0)
    pltpu.make_async_copy(wo_hbm, wo_ref, w_sem.at[3]).wait()

    keys_all = n_blk * n_u * rows

    def order(i):
        return jnp.where(i % 2 == 0, i // 2, last - i // 2)

    def c_right(o, src):
        return pltpu.make_async_remote_copy(
            src_ref=att.at[o, src], dst_ref=att.at[o, src],
            send_sem=sc_r.at[o, src], recv_sem=rc.at[o, src],
            device_id={"ulysses": z + 1}, device_id_type=MESH,
        )

    def c_left(o, src):
        return pltpu.make_async_remote_copy(
            src_ref=att.at[o, src], dst_ref=att.at[o, src],
            send_sem=sc_l.at[o, src], recv_sem=rc.at[o, src],
            device_id={"ulysses": z - 1}, device_id_type=MESH,
        )

    def d_copy(o, src):
        return pltpu.make_async_remote_copy(
            src_ref=stage.at[o], dst_ref=br.at[src],
            send_sem=sd.at[o], recv_sem=rd.at[src],
            device_id={"ulysses": o}, device_id_type=MESH,
        )

    group = 2 if n_u % 2 == 0 else 1

    def attend(chunks):
        for h in range(heads):
            keys = kv[0, h].reshape(keys_all, head)
            values = kv[1, h].reshape(keys_all, head)
            queries = jnp.concatenate(
                [q_ref[h, pl.ds(2 * o, 2)].reshape(rows, head) for o in chunks], axis=0
            )
            scores = lax.dot_general(
                queries, keys, (((1,), (1,)), ((), ())), preferred_element_type=F32
            )
            powers = jnp.exp(scores - jnp.max(scores, axis=-1, keepdims=True))
            total = jnp.sum(powers, axis=-1, keepdims=True)
            numerator = jnp.dot(powers.astype(BF), values, preferred_element_type=F32)
            result = (numerator / total).astype(BF)
            for g, o in enumerate(chunks):
                att[o, z, :, h * head:(h + 1) * head] = result[g * rows:(g + 1) * rows]

    def pass_right(o, src):
        c_right(o, src).wait_recv()

        @pl.when(z < last)
        def _():
            c_right(o, src).start()

    def pass_left(o, src):
        c_left(o, src).wait_recv()

        @pl.when(z > 0)
        def _():
            c_left(o, src).start()

    low = z < n_u // 2

    def attend_step(t, _):
        @pl.when(t < n_u // group)
        def _():
            chunks = [order(group * t + g) for g in range(group)]
            attend(chunks)
            for o in chunks:
                @pl.when(z < last)
                def _():
                    c_right(o, z).start()

                @pl.when(z > 0)
                def _():
                    c_left(o, z).start()

        for g in range(group):
            @pl.when((t > 0) & low & (z > 0))
            def _():
                pass_left(order(group * (t - 1) + g), z + 1)

            @pl.when((t > 0) & jnp.logical_not(low) & (z < last))
            def _():
                pass_right(order(group * (t - 1) + g), z - 1)

        return 0

    lax.fori_loop(0, n_u // group + 1, attend_step, 0)

    def mix_step(t, _):
        for k in range(last, 0, -1):
            i = t - k + 1
            held = (i >= 0) & (i < n_u)
            right_too = held & (z - k >= 0)
            left_too = held & (z + k <= last)
            if k == 1:
                right_too = right_too & (low | (z == last))
                left_too = left_too & (jnp.logical_not(low) | (z == 0))

            @pl.when(right_too)
            def _():
                pass_right(order(i), z - k)

            @pl.when(left_too)
            def _():
                pass_left(order(i), z + k)

        @pl.when(t >= last - 1)
        def _():
            o = order(t - last + 1)
            total = jnp.zeros((rows, width), F32)
            for src in range(n_u):
                total += jnp.dot(
                    att[o, src], wo_ref[src * width:(src + 1) * width, :],
                    preferred_element_type=F32,
                )

            @pl.when(o == z)
            def _():
                br[z] = total.astype(BF)

            @pl.when(o != z)
            def _():
                stage[o] = total.astype(BF)
                d_copy(o, z).start()

        return 0

    lax.fori_loop(0, n_u + last - 1, mix_step, 0)

    for src in range(n_u):
        @pl.when(src != z)
        def _():
            d_copy(src, src).wait_recv()

        cols = slice(src * width, (src + 1) * width)
        out_ref[:, cols] = (
            tok_ref[:, cols].astype(F32) + gate_ref[:, cols] * br[src].astype(F32)
        ).astype(BF)

    def finish(s, _):
        for u in range(2):
            @pl.when((s <= z) & (z < last))
            def _():
                a_right(2 * s + u).wait_send()

            @pl.when((s >= z) & (z > 0))
            def _():
                a_left(2 * s + u).wait_send()

        for src in range(n_u):
            @pl.when((src <= z) & (z < last))
            def _():
                c_right(s, src).wait_send()

            @pl.when((src >= z) & (z > 0))
            def _():
                c_left(s, src).wait_send()

        @pl.when(s != z)
        def _():
            d_copy(s, z).wait_send()

        for part in (0, 1):
            for mask in masks:
                for u in range(2):
                    b_copy(mask, part, 2 * s + u).wait_send()
        return 0

    lax.fori_loop(0, n_u, finish, 0)


def split_kernel(
    n_u, n_blk,
    tok_hbm, shift_hbm, scale_hbm, gate_hbm, w_hbm, qg_ref, kg_ref, wo_hbm, out_ref,
    w_ref, wo_ref, mod, q_ref, kv, wx_ref, att, xatt, stage, br,
    tok_ref, shift_ref, scale_ref, gate_ref, in_sem, swz, rwz, sw, rw, rw_core,
    w_sem, sa_r, sa_l, ra, sb, rb, rb_core, sq, rq, sx, rx, sc, rc, sd, rd,
):
    z = lax.axis_index("ulysses")
    b = lax.axis_index("blk")
    rows, model = tok_ref.shape
    head = qg_ref.shape[1]
    width = w_ref.shape[2]
    heads = width // head
    share = heads // 2
    cols = share * head
    factor = 1.0 / math.sqrt(head)
    last = n_u - 1
    half = rows // 2
    bits = [1 << i for i in range(n_blk.bit_length() - 1)]
    masks = range(1, n_blk)
    side = (b // SPLIT) % 2
    mine = side * share
    theirs = (1 - side) * share
    line_half = n_u // 2
    low = z < line_half
    hub = jnp.where(low, line_half - 1, line_half)
    is_hub = z == hub
    onward = jnp.where(low, 1, -1)
    away = jnp.where(low, hub - z, z - hub)
    slice_rows = model // n_blk
    part_rows = slice_rows // 2

    def flip(bit):
        return b + (1 - 2 * ((b // bit) % 2)) * bit

    barrier = pltpu.get_barrier_semaphore()
    for d in range(1, n_u):
        pl.semaphore_signal(
            barrier, inc=1, device_id={"ulysses": (z + d) % n_u}, device_id_type=MESH
        )
    for bit in bits:
        pl.semaphore_signal(barrier, inc=1, device_id={"blk": flip(bit)}, device_id_type=MESH)

    inputs = [
        pltpu.make_async_copy(src, dst, in_sem.at[i])
        for i, (src, dst) in enumerate((
            (tok_hbm, tok_ref), (shift_hbm, shift_ref), (scale_hbm, scale_ref), (gate_hbm, gate_ref),
        ))
    ]
    for copy in inputs:
        copy.start()
    for copy in inputs:
        copy.wait()
    def origin_of(mask):
        return b + sum((1 - 2 * ((b // bit) % 2)) * bit for bit in bits if mask & bit)

    slices = [
        pl.ds(pl.multiple_of(origin_of(mask) * slice_rows, 16), slice_rows) for mask in Z_MASKS
    ]
    wo_slices = [
        pltpu.make_async_copy(wo_hbm.at[rows_at], wo_ref.at[rows_at], w_sem.at[3 + i])
        for i, rows_at in enumerate(slices)
    ]
    wo_whole = pltpu.make_async_copy(wo_hbm, wo_ref, w_sem.at[3])

    @pl.when(jnp.logical_not(is_hub))
    def _():
        for copy in wo_slices:
            copy.start()

    for j in (1, 2, 0):
        pltpu.make_async_copy(w_hbm.at[j], w_ref.at[j], w_sem.at[j]).start()

    @pl.when(is_hub)
    def _():
        wo_whole.start()


    wide = tok_ref[...].astype(F32)
    center = jnp.mean(wide, axis=-1, keepdims=True)
    spread = jnp.mean((wide - center) ** 2, axis=-1, keepdims=True)
    normed = (wide - center) * lax.rsqrt(spread + 1e-06)
    modulated = (normed * (1.0 + scale_ref[...]) + shift_ref[...]).astype(BF)
    mod[pl.ds(2 * z, 2)] = modulated.reshape(2, half, model)

    with jax.named_scope("barrier"):
        pl.semaphore_wait(barrier, n_u - 1 + len(bits))

    def line_copy(buf, index, send, recv, step):
        return pltpu.make_async_remote_copy(
            src_ref=buf.at[index], dst_ref=buf.at[index],
            send_sem=send.at[index], recv_sem=recv.at[index],
            device_id={"ulysses": z + step}, device_id_type=MESH,
        )

    def a_right(o):
        return line_copy(mod, o, sa_r, ra, 1)

    def a_left(o):
        return line_copy(mod, o, sa_l, ra, -1)

    def drain(ref, sem):
        pltpu.make_async_copy(ref, ref, sem).wait()

    def rows_of(origin, part):
        return pl.ds(pl.multiple_of(origin * slice_rows + part * part_rows, 16), part_rows)

    def wz_copy(i, part, slot):
        origin = origin_of(Z_MASKS[i])
        return pltpu.make_async_remote_copy(
            src_ref=wo_ref.at[rows_of(origin, part)],
            dst_ref=wx_ref.at[slot, rows_of(origin, part)],
            send_sem=swz.at[i, part], recv_sem=rwz.at[slot, i, part],
            device_id={"ulysses": hub}, device_id_type=MESH,
        )

    def w_copy(mask, part):
        slot, bit = source_slot(mask, part)
        ref = wx_ref.at[:, rows_of(origin_of(slot), part)]
        return pltpu.make_async_remote_copy(
            src_ref=ref, dst_ref=ref,
            send_sem=sw, recv_sem=rw_core if mask & 1 else rw.at[mask // 2, part],
            device_id={"blk": flip(bit)}, device_id_type=MESH,
        )

    def w_wait(mask, part):
        ref = wx_ref.at[:, rows_of(origin_of(mask), part)]
        pltpu.make_async_remote_copy(
            src_ref=ref, dst_ref=ref,
            send_sem=sw, recv_sem=rw.at[mask // 2, part],
            device_id={"blk": flip(source_slot(mask, part)[1])}, device_id_type=MESH,
        ).wait_recv()

    def w_onward(mask, part):
        for later in sorted(masks, key=lambda m: m & 1):
            if source_slot(later, part)[0] == mask and later not in Z_MASKS:
                w_copy(later, part).start()

    def w_relay(mask, part):
        w_wait(mask, part)
        w_onward(mask, part)

    def w_arrived(i, part):
        for slot in range(line_half - 1):
            wz_copy(i, part, slot).wait_recv()

    def source(mask, part):
        if mask & 1:
            return mask - 1, 1
        if mask == SPLIT:
            return 0, SPLIT
        rest = mask & ~SPLIT
        bit = highest_bit(rest) if part == 0 else lowest_bit(rest)
        return mask - bit, bit

    def b_sem(mask, part, u):
        return rb_core if mask & 1 else rb.at[mask // 2 - 1, part, u]

    def b_copy(mask, part, u):
        slot, bit = source(mask, part)
        own = pl.ds(theirs if bit == SPLIT else mine, share)
        return pltpu.make_async_remote_copy(
            src_ref=kv.at[part, own, slot, u], dst_ref=kv.at[part, own, mask, u],
            send_sem=sb, recv_sem=b_sem(mask, part, u),
            device_id={"blk": flip(bit)}, device_id_type=MESH,
        )

    def b_cross(bit, part, u):
        own = pl.ds(theirs, share)
        return pltpu.make_async_remote_copy(
            src_ref=kv.at[part, own, 0, u], dst_ref=kv.at[part, own, SPLIT + bit, u],
            send_sem=sb, recv_sem=b_sem(SPLIT + bit, part, u),
            device_id={"blk": origin_of(SPLIT + bit)}, device_id_type=MESH,
        )

    def b_wait(mask, part, u):
        here = kv.at[part, pl.ds(mine, share), mask, u]
        pltpu.make_async_remote_copy(
            src_ref=here, dst_ref=here,
            send_sem=sb, recv_sem=b_sem(mask, part, u),
            device_id={"blk": flip(source(mask, part)[1])}, device_id_type=MESH,
        ).wait_recv()

    def q_copy(u, first):
        heads_of = pl.ds(first, share)
        return pltpu.make_async_remote_copy(
            src_ref=q_ref.at[heads_of, 0, u], dst_ref=q_ref.at[heads_of, 1, u],
            send_sem=sq, recv_sem=rq,
            device_id={"blk": flip(SPLIT)}, device_id_type=MESH,
        )

    def b_send(slot, part, u, cross=False):
        for mask in sorted(masks, key=lambda m: (m & 1, m != SPLIT)):
            at, bit = source(mask, part)
            if at == slot and not (cross and slot == SPLIT and bit != 1):
                b_copy(mask, part, u).start()
                if cross and mask == SPLIT:
                    for far_bit in bits[2:]:
                        b_cross(far_bit, part, u).start()

    def depth_of(mask):
        return bin(mask).count("1")

    def b_level(level, u, cross=False):
        for part in (0, 1):
            for mask in masks:
                if mask % 2 == 0 and depth_of(mask) == level:
                    b_wait(mask, part, u)
                    b_send(mask, part, u, cross)

    depth = len(bits) - 1

    def level_one(o):
        for u in range(2):
            b_level(1, 2 * o + u)

    def level_rest(o):
        for level in range(2, depth + 1):
            for u in range(2):
                b_level(level, 2 * o + u)

    def head_norm(sums, gain, scale):
        meansq = jnp.mean(sums * sums, axis=-1, keepdims=True)
        return sums * lax.rsqrt(meansq + 1e-06) * gain * scale

    def project(starts, count, own=False, between=None, cross=False):
        size = count * half

        def sums_of(j):
            if own:
                pltpu.make_async_copy(w_hbm.at[j], w_ref.at[j], w_sem.at[j]).wait()
            tokens = [mod[pl.ds(first, count)].reshape(size, model) for first in starts]
            sums = jnp.dot(
                jnp.concatenate(tokens, axis=0), w_ref[j], preferred_element_type=F32
            )
            return [sums[:, h * head:(h + 1) * head] for h in range(heads)]

        def put(value, at):
            for i, first in enumerate(starts):
                at(pl.ds(first, count), value[i * size:(i + 1) * size].reshape(count, half, head))

        def send(act):
            for first in starts:
                for u in range(count):
                    act(first + u)

        for h, sums in enumerate(sums_of(1)):
            def put_keys(units, part):
                kv[0, h, 0, units] = part
            put(head_norm(sums, kg_ref[...], 1.0).astype(BF), put_keys)
        send(lambda u: b_send(0, 0, u, cross))
        for h, sums in enumerate(sums_of(2)):
            def put_values(units, part):
                kv[1, h, 0, units] = part
            put(sums.astype(BF), put_values)
        send(lambda u: b_send(0, 1, u, cross))
        if between is not None:
            between()
        for h, sums in enumerate(sums_of(0)):
            def put_queries(units, part):
                q_ref[h, 0, units] = part
            put(head_norm(sums, qg_ref[...], factor).astype(BF), put_queries)
        send(lambda u: q_copy(u, theirs).start())

    for u in range(2):
        @pl.when(z < last)
        def _():
            a_right(2 * z + u).start()

        @pl.when(z > 0)
        def _():
            a_left(2 * z + u).start()

    @pl.when(jnp.logical_not(is_hub))
    def _():
        for i, copy in enumerate(wo_slices):
            copy.wait()
            for part in range(2):
                wz_copy(i, part, away - 1).start()

    def receive(k, u):
        @pl.when(z - k >= 0)
        def _():
            a_right(2 * (z - k) + u).wait_recv()

            @pl.when(z < last)
            def _():
                a_right(2 * (z - k) + u).start()

        @pl.when(z + k <= last)
        def _():
            a_left(2 * (z + k) + u).wait_recv()

            @pl.when(z > 0)
            def _():
                a_left(2 * (z + k) + u).start()

    def at_each(k, act):
        @pl.when(z >= k)
        def _():
            act(z - k)

        @pl.when((z + k <= last) & (k > 0))
        def _():
            act(z + k)

    def project_at(k, between):
        two = (z >= k) & (z + k <= last)

        @pl.when(two)
        def _():
            project([2 * (z - k), 2 * (z + k)], 2, between=between)

        @pl.when(jnp.logical_not(two) & ((z >= k) | (z + k <= last)))
        def _():
            project([2 * jnp.where(z >= k, z - k, z + k)], 2, between=between)

    with jax.named_scope("own"):
        project([2 * z], 2, own=True)
    receive(1, 0)
    level_one(z)
    if last > 1:
        receive(1, 1)

    def line_step(k, _):
        def between():
            @pl.when(k + 1 < last)
            def _():
                at_each(k - 1, level_rest)

        with jax.named_scope("project"):
            project_at(k, between)
        receive(k + 1, 0)

        @pl.when(k + 1 < last)
        def _():
            at_each(k, level_one)
            receive(k + 1, 1)

        return 0

    with jax.named_scope("line"):
        lax.fori_loop(1, last, line_step, 0)

    ends = (z == 0) | (z == last)
    far = last - z

    first_part = [(SPLIT, 0), (1, 0), (1, 1)]
    direct = [
        (mask, part) for part in (1, 0) for mask in masks
        if mask % 2 == 0 and mask != SPLIT and source_slot(mask, part)[0] == 0
    ]

    @pl.when(is_hub)
    def _():
        for part in range(2):
            w_arrived(0, part)
        for mask, part in first_part:
            w_copy(mask, part).start()

    with jax.named_scope("far"):
        @pl.when(jnp.logical_not(ends))
        def _():
            at_each(last - 1, level_one)
            at_each(last - 2, level_rest)
            at_each(last - 1, level_rest)

        def far_step(u, _):
            @pl.when(u == 1)
            def _():
                receive(last, 1)

            def between():
                @pl.when(u == 0)
                def _():
                    at_each(last - 1, level_one)

            with jax.named_scope("project_half"):
                project([2 * far + u], 1, between=between, cross=True)
            return 0

        @pl.when(ends)
        def _():
            lax.fori_loop(0, 2, far_step, 0)
            at_each(last - 2, level_rest)
            b_level(1, 2 * far, cross=True)
            at_each(last - 1, level_rest)
            b_level(1, 2 * far + 1, cross=True)
            for level in range(2, depth + 1):
                b_level(level, 2 * far, cross=True)
                b_level(level, 2 * far + 1, cross=True)

    @pl.when(is_hub)
    def _():
        for mask, part in direct:
            w_copy(mask, part).start()

    with jax.named_scope("b_finish"):
        drain(kv.at[:, pl.ds(0, share), pl.ds(0, n_blk // 2)], rb_core)
        drain(q_ref.at[pl.ds(0, share), 0], rq)

    keys_all = n_blk * n_u * rows

    def order(i, rightward):
        leftward = jnp.where(i < line_half, last - i, i - line_half)
        return jnp.where(rightward, last - leftward, leftward)

    def c_copy(o, src, sd):
        ref = att.at[o, src, :, pl.ds(pl.multiple_of(sd * cols, head), cols)]
        return pltpu.make_async_remote_copy(
            src_ref=ref, dst_ref=ref,
            send_sem=sc.at[src], recv_sem=rc.at[o, src, sd],
            device_id={"ulysses": z + onward}, device_id_type=MESH,
        )

    def c_send(t, sd):
        c_copy(order(t, low), z, sd).start()

    def x_copy(o, sd):
        return pltpu.make_async_remote_copy(
            src_ref=xatt.at[o],
            dst_ref=att.at[o, z, :, pl.ds(pl.multiple_of(sd * cols, head), cols)],
            send_sem=sx, recv_sem=rx.at[o],
            device_id={"blk": flip(SPLIT)}, device_id_type=MESH,
        )

    def quarter(d):
        return hub - onward * d

    def d_copy(o, d):
        return pltpu.make_async_remote_copy(
            src_ref=stage.at[o, d], dst_ref=br.at[quarter(d)],
            send_sem=sd, recv_sem=rd.at[quarter(d)],
            device_id={"ulysses": o}, device_id_type=MESH,
        )

    def attend(t):
        o = order(t, low)
        place = pl.multiple_of(side * cols, head)
        for r in range(share):
            h = mine + r
            keys = kv[0, h].reshape(keys_all, head)
            values = kv[1, h].reshape(keys_all, head)
            queries = jnp.concatenate(
                [q_ref[h, p, pl.ds(2 * o, 2)].reshape(rows, head) for p in range(2)], axis=0
            )
            scores = lax.dot_general(
                queries, keys, (((1,), (1,)), ((), ())), preferred_element_type=F32
            )
            powers = jnp.exp(scores - jnp.max(scores, axis=-1, keepdims=True))
            total = jnp.sum(powers, axis=-1, keepdims=True)
            numerator = jnp.dot(powers.astype(BF), values, preferred_element_type=F32)
            result = (numerator / total).astype(BF)
            att[o, z, :, pl.ds(pl.multiple_of(place + r * head, head), head)] = result[:rows]
            xatt[o, :, r * head:(r + 1) * head] = result[rows:]
        x_copy(o, side).start()
        c_send(t, side)

    def pass_on(i, k):
        src = z - onward * k
        there = (src >= 0) & (src <= last)

        @pl.when(there & (i >= 0) & (i < n_u))
        def _():
            copy = c_copy(order(i, low), src, side)
            copy.wait_recv()
            copy.start()

        @pl.when(there & (i >= 1) & (i <= n_u))
        def _():
            copy = c_copy(order(i - 1, low), src, 1 - side)
            copy.wait_recv()
            copy.start()

    def x_step(t):
        x_copy(order(t, low), 1 - side).wait_recv()
        c_send(t, 1 - side)

    def attend_step(t, _):
        with jax.named_scope("attend"):
            attend(t)

        @pl.when(is_hub & (t == n_u - 1))
        def _():
            w_copy(SPLIT, 1).start()

        @pl.when(t > 1)
        def _():
            x_step(t - 2)

        return 0

    with jax.named_scope("attend_loop"):
        lax.fori_loop(0, n_u, attend_step, 0)

        for t in range(max(n_u - 2, 0), n_u):
            x_step(t)

        @pl.when(is_hub)
        def _():
            w_relay(SPLIT, 0)
            w_relay(2 * SPLIT, 1)
            for part in range(2):
                w_arrived(1, part)
                w_onward(Z_MASKS[1], part)

    def mix(indices, weights, d):
        chunks = [order(i, jnp.logical_not(low)) for i in indices]
        with jax.named_scope("mix"):
            total = jnp.zeros((len(chunks) * rows, width), F32)
            for src in range(n_u):
                total += jnp.dot(
                    jnp.concatenate([att[o, src] for o in chunks], axis=0),
                    weights[src * width:(src + 1) * width, :],
                    preferred_element_type=F32,
                )
            result = total.astype(BF)
        for g, o in enumerate(chunks):
            part = result[g * rows:(g + 1) * rows]

            @pl.when(o == z)
            def _():
                br[quarter(d)] = part

            @pl.when(o != z)
            def _():
                stage[o, d] = part
                d_copy(o, d).start()

    def gathered(i):
        for k in range(line_half):
            for sd_of in (side, 1 - side):
                c_copy(order(i, jnp.logical_not(low)), hub + onward * (k + 1), sd_of).wait_recv()

    gap = 2
    steps = n_u + 1 + gap * (line_half - 2)

    def pass_step(t, _):
        for k in range(1, line_half):
            pass_on(t - gap * (k - 1), k)

        @pl.when(is_hub & (t == 2))
        def _():
            w_relay(SPLIT, 1)
            w_relay(2 * SPLIT, 0)

        i = t - (steps - line_half)

        @pl.when(is_hub & (i >= 0))
        def _():
            gathered(i)
            mix([i], wo_ref, 0)

        return 0

    with jax.named_scope("pass_loop"):
        @pl.when(is_hub)
        def _():
            wo_whole.wait()

        lax.fori_loop(0, steps, pass_step, 0)

    with jax.named_scope("hub"):
        @pl.when(is_hub)
        def _():
            with jax.named_scope("w_last"):
                for mask in sorted(masks, key=depth_of):
                    if mask % 2 == 0 and mask not in (SPLIT, 2 * SPLIT, *Z_MASKS):
                        for part in range(2):
                            w_relay(mask, part)
                drain(wx_ref.at[:, pl.ds(0, n_blk // 2 * slice_rows)], rw_core)

            for d in range(1, line_half):
                mix(range(line_half), wx_ref.at[d - 1], d)

            def near_mix(i, _):
                gathered(i)
                mix([i], wo_ref, 0)
                for d in range(1, line_half):
                    mix([i], wx_ref.at[d - 1], d)
                return 0

            lax.fori_loop(line_half, n_u, near_mix, 0)

    with jax.named_scope("final"):
        for src in range(n_u):
            @pl.when(jnp.logical_not(is_hub) | (low != (src < line_half)))
            def _():
                pltpu.make_async_remote_copy(
                    src_ref=br.at[src], dst_ref=br.at[src],
                    send_sem=rd.at[src], recv_sem=rd.at[src],
                    device_id={"ulysses": last - hub}, device_id_type=MESH,
                ).wait_recv()

            at = slice(src * width, (src + 1) * width)
            out_ref[:, at] = (
                tok_ref[:, at].astype(F32) + gate_ref[:, at] * br[src].astype(F32)
            ).astype(BF)

    def finish(s, _):
        for u in range(2):
            @pl.when((s <= z) & (z < last))
            def _():
                a_right(2 * s + u).wait_send()

            @pl.when((s >= z) & (z > 0))
            def _():
                a_left(2 * s + u).wait_send()

        @pl.when(jnp.where(low, s <= z, s >= z))
        def _():
            drain(att.at[:, s], sc.at[s])

        return 0

    with jax.named_scope("finish"):
        lax.fori_loop(0, n_u, finish, 0)

        drain(xatt, sx)
        drain(q_ref.at[pl.ds(0, share), 0], sq)
        drain(kv.at[:, pl.ds(0, share), pl.ds(1, n_blk - 1)], sb)

        @pl.when(is_hub)
        def _():
            drain(stage.at[pl.ds(0, n_u - 1)], sd)
            drain(wx_ref.at[:, pl.ds(0, (n_blk - len(Z_MASKS)) * slice_rows)], sw)

        @pl.when(jnp.logical_not(is_hub))
        def _():
            for i in range(len(Z_MASKS)):
                for part in range(2):
                    wz_copy(i, part, away - 1).wait_send()


def local(n_u, n_blk, tokens, mod_shift, mod_scale, mod_gate, qkv_weight, query_gain, key_gain, out_weight):
    rows, model = tokens.shape
    width = qkv_weight.shape[2]
    head = query_gain.shape[0]
    heads = width // head
    vmem = pl.BlockSpec(memory_space=pltpu.VMEM)
    hbm = pl.BlockSpec(memory_space=pltpu.HBM)
    dma = pltpu.SemaphoreType.DMA
    split = heads % 2 == 0 and n_blk % (4 * SPLIT) == 0 and n_u % 2 == 0 and n_u > 2
    buffers = [
        pltpu.VMEM(qkv_weight.shape, BF),
        pltpu.VMEM(out_weight.shape, BF),
        pltpu.VMEM((2 * n_u, rows // 2, model), BF),
    ]
    line_sems = [dma((4,)), dma((2 * n_u,)), dma((2 * n_u,)), dma((2 * n_u,))]
    block_sems = [dma((n_blk, 2, 2 * n_u)), dma((n_blk, 2, 2 * n_u))]
    keys = pltpu.VMEM((2, heads, n_blk, 2 * n_u, rows // 2, head), BF)
    attended = pltpu.VMEM((n_u, n_u, rows, width), BF)
    mixed = pltpu.VMEM((n_u, rows, width), BF)
    row = pltpu.VMEM((1, model), F32)
    early = hbm if split else vmem
    one = pltpu.SemaphoreType.DMA
    if split:
        body = split_kernel
        scratch = buffers + [
            pltpu.VMEM((heads, 2, 2 * n_u, rows // 2, head), BF), keys,
            pltpu.VMEM((n_u // 2 - 1, *out_weight.shape), BF),
            attended, pltpu.VMEM((n_u, rows, width // 2), BF),
            pltpu.VMEM((n_u, n_u // 2, rows, width), BF), mixed,
            pltpu.VMEM((rows, model), BF), row, row, row, dma((4,)),
            dma((2, 2)), dma((n_u // 2 - 1, 2, 2)), one, dma((n_blk // 2, 2)), one,
            dma((5,)),
        ] + line_sems[1:] + [
            one, dma((n_blk // 2 - 1, 2, 2 * n_u)), one, one, one, one, dma((n_u,)),
            dma((n_u,)), dma((n_u, n_u, 2)), one, dma((n_u,)),
        ]
    else:
        body = kernel
        scratch = buffers + [
            pltpu.VMEM((heads, 2 * n_u, rows // 2, head), BF), keys,
            attended, mixed, mixed,
        ] + line_sems + block_sems + [
            dma((n_u, n_u)), dma((n_u, n_u)), dma((n_u, n_u)),
            dma((n_u,)), dma((n_u,)),
        ]
    return pl.pallas_call(
        functools.partial(body, n_u, n_blk),
        out_shape=pltpu.VMEM((rows, model), BF) if split else jax.ShapeDtypeStruct((rows, model), BF),
        in_specs=[early, early, early, early, hbm, vmem, vmem, hbm],
        out_specs=vmem,
        scratch_shapes=scratch,
        compiler_params=pltpu.CompilerParams(
            collective_id=0, has_side_effects=True, vmem_limit_bytes=63_000_000 if split else 66_000_000
        ),
    )(
        tokens, mod_shift[None], mod_scale[None], mod_gate[None],
        qkv_weight, query_gain[None], key_gain[None], out_weight,
    )


def solution(mesh):
    in_specs = (
        P(("blk", "ulysses"), None), P(), P(), P(),
        P(None, None, "ulysses"), P(), P(), P(None, "ulysses"),
    )
    out_specs = P(("blk", "ulysses"), None)
    body = functools.partial(local, mesh.shape["ulysses"], mesh.shape["blk"])
    return jax.shard_map(body, mesh=mesh, in_specs=in_specs, out_specs=out_specs, check_vma=False)
```

```python
import functools
import math

import jax
import jax.numpy as jnp
from jax import lax
from jax.experimental import pallas as pl
from jax.experimental.pallas import tpu as pltpu
from jax.sharding import PartitionSpec as P

MESH = pl.DeviceIdType.MESH
BF = jnp.bfloat16
F32 = jnp.float32
SPLIT = 2
Z_MASKS = (0, 3 * SPLIT)


def highest_bit(mask):
    return 1 << (mask.bit_length() - 1)


def lowest_bit(mask):
    return mask & -mask


def source_slot(mask, part):
    if mask & 1:
        return mask - 1, 1
    bit = highest_bit(mask) if part == 0 else lowest_bit(mask)
    return mask - bit, bit


def kernel(
    n_u, n_blk,
    tok_ref, shift_ref, scale_ref, gate_ref, w_hbm, qg_ref, kg_ref, wo_hbm, out_ref,
    w_ref, wo_ref, mod, q_ref, kv, att, stage, br,
    w_sem, sa_r, sa_l, ra, sb, rb, sc_r, sc_l, rc, sd, rd,
):
    z = lax.axis_index("ulysses")
    b = lax.axis_index("blk")
    rows, model = tok_ref.shape
    head = qg_ref.shape[1]
    width = w_ref.shape[2]
    heads = width // head
    factor = 1.0 / math.sqrt(head)
    last = n_u - 1
    half = rows // 2
    bits = [1 << i for i in range(n_blk.bit_length() - 1)]
    pair = 2 if heads % 2 == 0 else heads
    tile = pair * head

    for j in (1, 2, 0):
        pltpu.make_async_copy(w_hbm.at[j], w_ref.at[j], w_sem.at[j]).start()
    pltpu.make_async_copy(wo_hbm, wo_ref, w_sem.at[3]).start()

    def flip(bit):
        return b + (1 - 2 * ((b // bit) % 2)) * bit

    barrier = pltpu.get_barrier_semaphore()
    for d in range(1, n_u):
        pl.semaphore_signal(
            barrier, inc=1, device_id={"ulysses": (z + d) % n_u}, device_id_type=MESH
        )
    for bit in bits:
        pl.semaphore_signal(barrier, inc=1, device_id={"blk": flip(bit)}, device_id_type=MESH)

    wide = tok_ref[...].astype(F32)
    center = jnp.mean(wide, axis=-1, keepdims=True)
    spread = jnp.mean((wide - center) ** 2, axis=-1, keepdims=True)
    normed = (wide - center) * lax.rsqrt(spread + 1e-06)
    modulated = (normed * (1.0 + scale_ref[...]) + shift_ref[...]).astype(BF)
    mod[pl.ds(2 * z, 2)] = modulated.reshape(2, half, model)

    pl.semaphore_wait(barrier, n_u - 1 + len(bits))

    def line_copy(buf, index, send, recv, step):
        return pltpu.make_async_remote_copy(
            src_ref=buf.at[index], dst_ref=buf.at[index],
            send_sem=send.at[index], recv_sem=recv.at[index],
            device_id={"ulysses": z + step}, device_id_type=MESH,
        )

    def a_right(o):
        return line_copy(mod, o, sa_r, ra, 1)

    def a_left(o):
        return line_copy(mod, o, sa_l, ra, -1)

    def b_copy(mask, part, s):
        slot, bit = source_slot(mask, part)
        return pltpu.make_async_remote_copy(
            src_ref=kv.at[part, :, slot, s], dst_ref=kv.at[part, :, mask, s],
            send_sem=sb.at[mask, part, s], recv_sem=rb.at[mask, part, s],
            device_id={"blk": flip(bit)}, device_id_type=MESH,
        )

    masks = range(1, n_blk)

    def b_send(slot, part, s):
        for mask in sorted(masks, key=lambda m: m & 1):
            if source_slot(mask, part)[0] == slot:
                b_copy(mask, part, s).start()

    def b_level(level, s):
        for part in (0, 1):
            for mask in masks:
                if mask % 2 == 0 and bin(mask).count("1") == level:
                    b_copy(mask, part, s).wait_recv()
                    b_send(mask, part, s)

    levels = range(1, len(bits))

    def head_norm(sums, gain, scale):
        meansq = jnp.mean(sums * sums, axis=-1, keepdims=True)
        return sums * lax.rsqrt(meansq + 1e-06) * gain * scale

    def project(j, first, count, put):
        def body(i, _):
            start = pl.multiple_of(i * tile, tile)
            sums = jnp.dot(
                mod[pl.ds(first, count)].reshape(count * half, model),
                w_ref[j, :, pl.ds(start, tile)],
                preferred_element_type=F32,
            )
            for e in range(pair):
                put(i * pair + e, sums[:, e * head:(e + 1) * head])
            return 0

        lax.fori_loop(0, heads // pair, body, 0)

    def project_chunk(first, count, own=False):
        units = pl.ds(first, count)

        def ready(j):
            if own:
                pltpu.make_async_copy(w_hbm.at[j], w_ref.at[j], w_sem.at[j]).wait()

        def put_key(h, sums):
            keys = head_norm(sums, kg_ref[...], 1.0).astype(BF)
            kv[0, h, 0, units] = keys.reshape(count, half, head)

        def put_value(h, sums):
            kv[1, h, 0, units] = sums.astype(BF).reshape(count, half, head)

        def put_query(h, sums):
            queries = head_norm(sums, qg_ref[...], factor).astype(BF)
            q_ref[h, units] = queries.reshape(count, half, head)

        ready(1)
        project(1, first, count, put_key)
        for u in range(count):
            b_send(0, 0, first + u)
        ready(2)
        project(2, first, count, put_value)
        for u in range(count):
            b_send(0, 1, first + u)
        ready(0)
        project(0, first, count, put_query)

    for u in range(2):
        @pl.when(z < last)
        def _():
            a_right(2 * z + u).start()

        @pl.when(z > 0)
        def _():
            a_left(2 * z + u).start()

    project_chunk(2 * z, 2, own=True)

    def at_distance(k, act):
        for side in (-1, 1):
            o = z + side * k

            @pl.when((o >= 0) & (o <= last))
            def _():
                act(o)

    def pass_levels(which):
        def act(o):
            for level in which:
                for u in range(2):
                    b_level(level, 2 * o + u)
        return act

    def receive(k):
        for u in range(2):
            @pl.when(z - k >= 0)
            def _():
                a_right(2 * (z - k) + u).wait_recv()

                @pl.when(z < last)
                def _():
                    a_right(2 * (z - k) + u).start()

            @pl.when(z + k <= last)
            def _():
                a_left(2 * (z + k) + u).wait_recv()

                @pl.when(z > 0)
                def _():
                    a_left(2 * (z + k) + u).start()

    def previous(k, which):
        if isinstance(k, int) and k == 1:
            pass_levels(which)(z)
        else:
            at_distance(k - 1, pass_levels(which))

    for k in range(1, last):
        receive(k)
        previous(k, levels[:1])
        at_distance(k, lambda o: project_chunk(2 * o, 2))
        previous(k, levels[1:])

    ends = (z == 0) | (z == last)
    far = last - z

    def far_half(u):
        @pl.when(ends)
        def _():
            @pl.when(z == 0)
            def _():
                a_left(2 * far + u).wait_recv()

            @pl.when(z > 0)
            def _():
                a_right(2 * far + u).wait_recv()

            project_chunk(2 * far + u, 1)

    def far_levels(u, which):
        @pl.when(ends)
        def _():
            for level in which:
                b_level(level, 2 * far + u)

    previous(last, levels[:1])
    far_half(0)
    previous(last, levels[1:])
    far_levels(0, levels[:1])
    far_half(1)
    far_levels(0, levels[1:])
    far_levels(1, levels)

    def b_finish(s, _):
        for part in (0, 1):
            for mask in masks:
                if mask % 2 == 1:
                    b_copy(mask, part, s).wait_recv()
        return 0

    lax.fori_loop(0, 2 * n_u, b_finish, 0)
    pltpu.make_async_copy(wo_hbm, wo_ref, w_sem.at[3]).wait()

    keys_all = n_blk * n_u * rows

    def order(i):
        return jnp.where(i % 2 == 0, i // 2, last - i // 2)

    def c_right(o, src):
        return pltpu.make_async_remote_copy(
            src_ref=att.at[o, src], dst_ref=att.at[o, src],
            send_sem=sc_r.at[o, src], recv_sem=rc.at[o, src],
            device_id={"ulysses": z + 1}, device_id_type=MESH,
        )

    def c_left(o, src):
        return pltpu.make_async_remote_copy(
            src_ref=att.at[o, src], dst_ref=att.at[o, src],
            send_sem=sc_l.at[o, src], recv_sem=rc.at[o, src],
            device_id={"ulysses": z - 1}, device_id_type=MESH,
        )

    def d_copy(o, src):
        return pltpu.make_async_remote_copy(
            src_ref=stage.at[o], dst_ref=br.at[src],
            send_sem=sd.at[o], recv_sem=rd.at[src],
            device_id={"ulysses": o}, device_id_type=MESH,
        )

    group = 2 if n_u % 2 == 0 else 1

    def attend(chunks):
        for h in range(heads):
            keys = kv[0, h].reshape(keys_all, head)
            values = kv[1, h].reshape(keys_all, head)
            queries = jnp.concatenate(
                [q_ref[h, pl.ds(2 * o, 2)].reshape(rows, head) for o in chunks], axis=0
            )
            scores = lax.dot_general(
                queries, keys, (((1,), (1,)), ((), ())), preferred_element_type=F32
            )
            powers = jnp.exp(scores - jnp.max(scores, axis=-1, keepdims=True))
            total = jnp.sum(powers, axis=-1, keepdims=True)
            numerator = jnp.dot(powers.astype(BF), values, preferred_element_type=F32)
            result = (numerator / total).astype(BF)
            for g, o in enumerate(chunks):
                att[o, z, :, h * head:(h + 1) * head] = result[g * rows:(g + 1) * rows]

    def pass_right(o, src):
        c_right(o, src).wait_recv()

        @pl.when(z < last)
        def _():
            c_right(o, src).start()

    def pass_left(o, src):
        c_left(o, src).wait_recv()

        @pl.when(z > 0)
        def _():
            c_left(o, src).start()

    low = z < n_u // 2

    def attend_step(t, _):
        @pl.when(t < n_u // group)
        def _():
            chunks = [order(group * t + g) for g in range(group)]
            attend(chunks)
            for o in chunks:
                @pl.when(z < last)
                def _():
                    c_right(o, z).start()

                @pl.when(z > 0)
                def _():
                    c_left(o, z).start()

        for g in range(group):
            @pl.when((t > 0) & low & (z > 0))
            def _():
                pass_left(order(group * (t - 1) + g), z + 1)

            @pl.when((t > 0) & jnp.logical_not(low) & (z < last))
            def _():
                pass_right(order(group * (t - 1) + g), z - 1)

        return 0

    lax.fori_loop(0, n_u // group + 1, attend_step, 0)

    def mix_step(t, _):
        for k in range(last, 0, -1):
            i = t - k + 1
            held = (i >= 0) & (i < n_u)
            right_too = held & (z - k >= 0)
            left_too = held & (z + k <= last)
            if k == 1:
                right_too = right_too & (low | (z == last))
                left_too = left_too & (jnp.logical_not(low) | (z == 0))

            @pl.when(right_too)
            def _():
                pass_right(order(i), z - k)

            @pl.when(left_too)
            def _():
                pass_left(order(i), z + k)

        @pl.when(t >= last - 1)
        def _():
            o = order(t - last + 1)
            total = jnp.zeros((rows, width), F32)
            for src in range(n_u):
                total += jnp.dot(
                    att[o, src], wo_ref[src * width:(src + 1) * width, :],
                    preferred_element_type=F32,
                )

            @pl.when(o == z)
            def _():
                br[z] = total.astype(BF)

            @pl.when(o != z)
            def _():
                stage[o] = total.astype(BF)
                d_copy(o, z).start()

        return 0

    lax.fori_loop(0, n_u + last - 1, mix_step, 0)

    for src in range(n_u):
        @pl.when(src != z)
        def _():
            d_copy(src, src).wait_recv()

        cols = slice(src * width, (src + 1) * width)
        out_ref[:, cols] = (
            tok_ref[:, cols].astype(F32) + gate_ref[:, cols] * br[src].astype(F32)
        ).astype(BF)

    def finish(s, _):
        for u in range(2):
            @pl.when((s <= z) & (z < last))
            def _():
                a_right(2 * s + u).wait_send()

            @pl.when((s >= z) & (z > 0))
            def _():
                a_left(2 * s + u).wait_send()

        for src in range(n_u):
            @pl.when((src <= z) & (z < last))
            def _():
                c_right(s, src).wait_send()

            @pl.when((src >= z) & (z > 0))
            def _():
                c_left(s, src).wait_send()

        @pl.when(s != z)
        def _():
            d_copy(s, z).wait_send()

        for part in (0, 1):
            for mask in masks:
                for u in range(2):
                    b_copy(mask, part, 2 * s + u).wait_send()
        return 0

    lax.fori_loop(0, n_u, finish, 0)


def split_kernel(
    n_u, n_blk,
    tok_hbm, shift_hbm, scale_hbm, gate_hbm, w_hbm, qg_ref, kg_ref, wo_hbm, out_ref,
    w_ref, wo_ref, mod, q_ref, kv, wx_ref, att, xatt, stage, br,
    tok_ref, shift_ref, scale_ref, gate_ref, in_sem, swz, rwz, sw, rw, rw_core,
    w_sem, sa_r, sa_l, ra, sb, rb, rb_core, sq, rq, sx, rx, sc, rc, sd, rd,
):
    z = lax.axis_index("ulysses")
    b = lax.axis_index("blk")
    rows, model = tok_ref.shape
    head = qg_ref.shape[1]
    width = w_ref.shape[2]
    heads = width // head
    share = heads // 2
    cols = share * head
    factor = 1.0 / math.sqrt(head)
    last = n_u - 1
    half = rows // 2
    bits = [1 << i for i in range(n_blk.bit_length() - 1)]
    masks = range(1, n_blk)
    side = (b // SPLIT) % 2
    mine = side * share
    theirs = (1 - side) * share
    line_half = n_u // 2
    low = z < line_half
    hub = jnp.where(low, line_half - 1, line_half)
    is_hub = z == hub
    onward = jnp.where(low, 1, -1)
    away = jnp.where(low, hub - z, z - hub)
    slice_rows = model // n_blk
    part_rows = slice_rows // 2

    def flip(bit):
        return b + (1 - 2 * ((b // bit) % 2)) * bit

    barrier = pltpu.get_barrier_semaphore()
    for d in range(1, n_u):
        pl.semaphore_signal(
            barrier, inc=1, device_id={"ulysses": (z + d) % n_u}, device_id_type=MESH
        )
    for bit in bits:
        pl.semaphore_signal(barrier, inc=1, device_id={"blk": flip(bit)}, device_id_type=MESH)

    inputs = [
        pltpu.make_async_copy(src, dst, in_sem.at[i])
        for i, (src, dst) in enumerate((
            (tok_hbm, tok_ref), (shift_hbm, shift_ref), (scale_hbm, scale_ref), (gate_hbm, gate_ref),
        ))
    ]
    for copy in inputs:
        copy.start()
    for copy in inputs:
        copy.wait()
    def origin_of(mask):
        return b + sum((1 - 2 * ((b // bit) % 2)) * bit for bit in bits if mask & bit)

    slices = [
        pl.ds(pl.multiple_of(origin_of(mask) * slice_rows, 16), slice_rows) for mask in Z_MASKS
    ]
    wo_slices = [
        pltpu.make_async_copy(wo_hbm.at[rows_at], wo_ref.at[rows_at], w_sem.at[3 + i])
        for i, rows_at in enumerate(slices)
    ]
    wo_whole = pltpu.make_async_copy(wo_hbm, wo_ref, w_sem.at[3])

    @pl.when(jnp.logical_not(is_hub))
    def _():
        for copy in wo_slices:
            copy.start()

    for j in (1, 2, 0):
        pltpu.make_async_copy(w_hbm.at[j], w_ref.at[j], w_sem.at[j]).start()

    @pl.when(is_hub)
    def _():
        wo_whole.start()


    wide = tok_ref[...].astype(F32)
    center = jnp.mean(wide, axis=-1, keepdims=True)
    spread = jnp.mean((wide - center) ** 2, axis=-1, keepdims=True)
    normed = (wide - center) * lax.rsqrt(spread + 1e-06)
    modulated = (normed * (1.0 + scale_ref[...]) + shift_ref[...]).astype(BF)
    mod[pl.ds(2 * z, 2)] = modulated.reshape(2, half, model)

    with jax.named_scope("barrier"):
        pl.semaphore_wait(barrier, n_u - 1 + len(bits))

    def line_copy(buf, index, send, recv, step):
        return pltpu.make_async_remote_copy(
            src_ref=buf.at[index], dst_ref=buf.at[index],
            send_sem=send.at[index], recv_sem=recv.at[index],
            device_id={"ulysses": z + step}, device_id_type=MESH,
        )

    def a_right(o):
        return line_copy(mod, o, sa_r, ra, 1)

    def a_left(o):
        return line_copy(mod, o, sa_l, ra, -1)

    def drain(ref, sem):
        pltpu.make_async_copy(ref, ref, sem).wait()

    def rows_of(origin, part):
        return pl.ds(pl.multiple_of(origin * slice_rows + part * part_rows, 16), part_rows)

    def wz_copy(i, part, slot):
        origin = origin_of(Z_MASKS[i])
        return pltpu.make_async_remote_copy(
            src_ref=wo_ref.at[rows_of(origin, part)],
            dst_ref=wx_ref.at[slot, rows_of(origin, part)],
            send_sem=swz.at[i, part], recv_sem=rwz.at[slot, i, part],
            device_id={"ulysses": hub}, device_id_type=MESH,
        )

    def w_copy(mask, part):
        slot, bit = source_slot(mask, part)
        ref = wx_ref.at[:, rows_of(origin_of(slot), part)]
        return pltpu.make_async_remote_copy(
            src_ref=ref, dst_ref=ref,
            send_sem=sw, recv_sem=rw_core if mask & 1 else rw.at[mask // 2, part],
            device_id={"blk": flip(bit)}, device_id_type=MESH,
        )

    def w_wait(mask, part):
        ref = wx_ref.at[:, rows_of(origin_of(mask), part)]
        pltpu.make_async_remote_copy(
            src_ref=ref, dst_ref=ref,
            send_sem=sw, recv_sem=rw.at[mask // 2, part],
            device_id={"blk": flip(source_slot(mask, part)[1])}, device_id_type=MESH,
        ).wait_recv()

    def w_onward(mask, part):
        for later in sorted(masks, key=lambda m: m & 1):
            if source_slot(later, part)[0] == mask and later not in Z_MASKS:
                w_copy(later, part).start()

    def w_relay(mask, part):
        w_wait(mask, part)
        w_onward(mask, part)

    def w_arrived(i, part):
        for slot in range(line_half - 1):
            wz_copy(i, part, slot).wait_recv()

    def source(mask, part):
        if mask & 1:
            return mask - 1, 1
        if mask == SPLIT:
            return 0, SPLIT
        rest = mask & ~SPLIT
        bit = highest_bit(rest) if part == 0 else lowest_bit(rest)
        return mask - bit, bit

    def b_sem(mask, part, u, count):
        at = u // 2 if count == 2 else jnp.where(u % 2 == 0, u // 2, n_u)
        return rb_core if mask & 1 else rb.at[mask // 2 - 1, part, at]

    def b_copy(mask, part, u, count):
        units = pl.ds(u, count)
        slot, bit = source(mask, part)
        own = pl.ds(theirs if bit == SPLIT else mine, share)
        return pltpu.make_async_remote_copy(
            src_ref=kv.at[part, own, slot, units], dst_ref=kv.at[part, own, mask, units],
            send_sem=sb, recv_sem=b_sem(mask, part, u, count),
            device_id={"blk": flip(bit)}, device_id_type=MESH,
        )

    def b_cross(bit, part, u, count):
        units = pl.ds(u, count)
        own = pl.ds(theirs, share)
        return pltpu.make_async_remote_copy(
            src_ref=kv.at[part, own, 0, units], dst_ref=kv.at[part, own, SPLIT + bit, units],
            send_sem=sb, recv_sem=b_sem(SPLIT + bit, part, u, count),
            device_id={"blk": origin_of(SPLIT + bit)}, device_id_type=MESH,
        )

    def b_wait(mask, part, u, count):
        here = kv.at[part, pl.ds(mine, share), mask, pl.ds(u, count)]
        pltpu.make_async_remote_copy(
            src_ref=here, dst_ref=here,
            send_sem=sb, recv_sem=b_sem(mask, part, u, count),
            device_id={"blk": flip(source(mask, part)[1])}, device_id_type=MESH,
        ).wait_recv()

    def q_copy(u, first, count):
        heads_of = pl.ds(first, share)
        return pltpu.make_async_remote_copy(
            src_ref=q_ref.at[heads_of, 0, pl.ds(u, count)],
            dst_ref=q_ref.at[heads_of, 1, pl.ds(u, count)],
            send_sem=sq, recv_sem=rq,
            device_id={"blk": flip(SPLIT)}, device_id_type=MESH,
        )

    def b_send(slot, part, u, count, cross=False):
        for mask in sorted(masks, key=lambda m: (m & 1, m != SPLIT)):
            at, bit = source(mask, part)
            if at == slot and not (cross and slot == SPLIT and bit != 1):
                b_copy(mask, part, u, count).start()
                if cross and mask == SPLIT:
                    for far_bit in bits[2:]:
                        b_cross(far_bit, part, u, count).start()

    def depth_of(mask):
        return bin(mask).count("1")

    def b_level(level, u, count=1, cross=False):
        for part in (0, 1):
            for mask in masks:
                if mask % 2 == 0 and depth_of(mask) == level:
                    b_wait(mask, part, u, count)
                    b_send(mask, part, u, count, cross)

    depth = len(bits) - 1

    def level_one(o):
        b_level(1, 2 * o, 2)

    def level_rest(o):
        for level in range(2, depth + 1):
            b_level(level, 2 * o, 2)

    def head_norm(sums, gain, scale):
        meansq = jnp.mean(sums * sums, axis=-1, keepdims=True)
        return sums * lax.rsqrt(meansq + 1e-06) * gain * scale

    def project(starts, count, own=False, between=None, cross=False):
        size = count * half

        def sums_of(j):
            if own:
                pltpu.make_async_copy(w_hbm.at[j], w_ref.at[j], w_sem.at[j]).wait()
            tokens = [mod[pl.ds(first, count)].reshape(size, model) for first in starts]
            sums = jnp.dot(
                jnp.concatenate(tokens, axis=0), w_ref[j], preferred_element_type=F32
            )
            return [sums[:, h * head:(h + 1) * head] for h in range(heads)]

        def put(value, at):
            for i, first in enumerate(starts):
                at(pl.ds(first, count), value[i * size:(i + 1) * size].reshape(count, half, head))

        def send(act):
            for first in starts:
                act(first)

        for h, sums in enumerate(sums_of(1)):
            def put_keys(units, part):
                kv[0, h, 0, units] = part
            put(head_norm(sums, kg_ref[...], 1.0).astype(BF), put_keys)
        send(lambda u: b_send(0, 0, u, count, cross))
        for h, sums in enumerate(sums_of(2)):
            def put_values(units, part):
                kv[1, h, 0, units] = part
            put(sums.astype(BF), put_values)
        send(lambda u: b_send(0, 1, u, count, cross))
        if between is not None:
            between()
        for h, sums in enumerate(sums_of(0)):
            def put_queries(units, part):
                q_ref[h, 0, units] = part
            put(head_norm(sums, qg_ref[...], factor).astype(BF), put_queries)
        send(lambda u: q_copy(u, theirs, count).start())

    for u in range(2):
        @pl.when(z < last)
        def _():
            a_right(2 * z + u).start()

        @pl.when(z > 0)
        def _():
            a_left(2 * z + u).start()

    @pl.when(jnp.logical_not(is_hub))
    def _():
        for i, copy in enumerate(wo_slices):
            copy.wait()
            for part in range(2):
                wz_copy(i, part, away - 1).start()

    def receive(k, u):
        @pl.when(z - k >= 0)
        def _():
            a_right(2 * (z - k) + u).wait_recv()

            @pl.when(z < last)
            def _():
                a_right(2 * (z - k) + u).start()

        @pl.when(z + k <= last)
        def _():
            a_left(2 * (z + k) + u).wait_recv()

            @pl.when(z > 0)
            def _():
                a_left(2 * (z + k) + u).start()

    def at_each(k, act):
        @pl.when(z >= k)
        def _():
            act(z - k)

        @pl.when((z + k <= last) & (k > 0))
        def _():
            act(z + k)

    def project_at(k, between):
        two = (z >= k) & (z + k <= last)

        @pl.when(two)
        def _():
            project([2 * (z - k), 2 * (z + k)], 2, between=between)

        @pl.when(jnp.logical_not(two) & ((z >= k) | (z + k <= last)))
        def _():
            project([2 * jnp.where(z >= k, z - k, z + k)], 2, between=between)

    with jax.named_scope("own"):
        project([2 * z], 2, own=True)
    receive(1, 0)
    level_one(z)
    if last > 1:
        receive(1, 1)

    def line_step(k, _):
        def between():
            @pl.when(k + 1 < last)
            def _():
                at_each(k - 1, level_rest)

        with jax.named_scope("project"):
            project_at(k, between)
        receive(k + 1, 0)

        @pl.when(k + 1 < last)
        def _():
            at_each(k, level_one)
            receive(k + 1, 1)

        return 0

    with jax.named_scope("line"):
        lax.fori_loop(1, last, line_step, 0)

    ends = (z == 0) | (z == last)
    far = last - z

    first_part = [(SPLIT, 0), (1, 0), (1, 1)]
    direct = [
        (mask, part) for part in (1, 0) for mask in masks
        if mask % 2 == 0 and mask != SPLIT and source_slot(mask, part)[0] == 0
    ]

    @pl.when(is_hub)
    def _():
        for part in range(2):
            w_arrived(0, part)
        for mask, part in first_part:
            w_copy(mask, part).start()

    with jax.named_scope("far"):
        @pl.when(jnp.logical_not(ends))
        def _():
            at_each(last - 1, level_one)
            at_each(last - 2, level_rest)
            at_each(last - 1, level_rest)

        def far_step(u, _):
            @pl.when(u == 1)
            def _():
                receive(last, 1)

            def between():
                @pl.when(u == 0)
                def _():
                    at_each(last - 1, level_one)

            with jax.named_scope("project_half"):
                project([2 * far + u], 1, between=between, cross=True)
            return 0

        @pl.when(ends)
        def _():
            lax.fori_loop(0, 2, far_step, 0)
            at_each(last - 2, level_rest)
            b_level(1, 2 * far, cross=True)
            at_each(last - 1, level_rest)
            b_level(1, 2 * far + 1, cross=True)
            for level in range(2, depth + 1):
                b_level(level, 2 * far, cross=True)
                b_level(level, 2 * far + 1, cross=True)

    @pl.when(is_hub)
    def _():
        for mask, part in direct:
            w_copy(mask, part).start()

    with jax.named_scope("b_finish"):
        drain(kv.at[:, pl.ds(0, share), pl.ds(0, n_blk // 2)], rb_core)
        drain(q_ref.at[pl.ds(0, share), 0], rq)

    keys_all = n_blk * n_u * rows

    def order(i, rightward):
        leftward = jnp.where(i < line_half, last - i, i - line_half)
        return jnp.where(rightward, last - leftward, leftward)

    def c_copy(o, src, sd):
        ref = att.at[o, src, :, pl.ds(pl.multiple_of(sd * cols, head), cols)]
        return pltpu.make_async_remote_copy(
            src_ref=ref, dst_ref=ref,
            send_sem=sc.at[src], recv_sem=rc.at[o, src, sd],
            device_id={"ulysses": z + onward}, device_id_type=MESH,
        )

    def c_send(t, sd):
        c_copy(order(t, low), z, sd).start()

    def x_copy(o, sd):
        return pltpu.make_async_remote_copy(
            src_ref=xatt.at[o],
            dst_ref=att.at[o, z, :, pl.ds(pl.multiple_of(sd * cols, head), cols)],
            send_sem=sx, recv_sem=rx.at[o],
            device_id={"blk": flip(SPLIT)}, device_id_type=MESH,
        )

    def quarter(d):
        return hub - onward * d

    def d_copy(o, d):
        return pltpu.make_async_remote_copy(
            src_ref=stage.at[o, d], dst_ref=br.at[quarter(d)],
            send_sem=sd, recv_sem=rd.at[quarter(d)],
            device_id={"ulysses": o}, device_id_type=MESH,
        )

    def attend(t):
        o = order(t, low)
        place = pl.multiple_of(side * cols, head)
        for r in range(share):
            h = mine + r
            keys = kv[0, h].reshape(keys_all, head)
            values = kv[1, h].reshape(keys_all, head)
            queries = jnp.concatenate(
                [q_ref[h, p, pl.ds(2 * o, 2)].reshape(rows, head) for p in range(2)], axis=0
            )
            scores = lax.dot_general(
                queries, keys, (((1,), (1,)), ((), ())), preferred_element_type=F32
            )
            powers = jnp.exp(scores - jnp.max(scores, axis=-1, keepdims=True))
            total = jnp.sum(powers, axis=-1, keepdims=True)
            numerator = jnp.dot(powers.astype(BF), values, preferred_element_type=F32)
            result = (numerator / total).astype(BF)
            att[o, z, :, pl.ds(pl.multiple_of(place + r * head, head), head)] = result[:rows]
            xatt[o, :, r * head:(r + 1) * head] = result[rows:]
        x_copy(o, side).start()
        c_send(t, side)

    def pass_on(i, k):
        src = z - onward * k
        there = (src >= 0) & (src <= last)

        @pl.when(there & (i >= 0) & (i < n_u))
        def _():
            copy = c_copy(order(i, low), src, side)
            copy.wait_recv()
            copy.start()

        @pl.when(there & (i >= 1) & (i <= n_u))
        def _():
            copy = c_copy(order(i - 1, low), src, 1 - side)
            copy.wait_recv()
            copy.start()

    def x_step(t):
        x_copy(order(t, low), 1 - side).wait_recv()
        c_send(t, 1 - side)

    def attend_step(t, _):
        with jax.named_scope("attend"):
            attend(t)

        @pl.when(is_hub & (t == n_u - 1))
        def _():
            w_copy(SPLIT, 1).start()

        @pl.when(t > 1)
        def _():
            x_step(t - 2)

        return 0

    with jax.named_scope("attend_loop"):
        lax.fori_loop(0, n_u, attend_step, 0)

        for t in range(max(n_u - 2, 0), n_u):
            x_step(t)

        @pl.when(is_hub)
        def _():
            w_relay(SPLIT, 0)
            w_relay(2 * SPLIT, 1)
            for part in range(2):
                w_arrived(1, part)
                w_onward(Z_MASKS[1], part)

    def mix(indices, weights, d):
        chunks = [order(i, jnp.logical_not(low)) for i in indices]
        with jax.named_scope("mix"):
            total = jnp.zeros((len(chunks) * rows, width), F32)
            for src in range(n_u):
                total += jnp.dot(
                    jnp.concatenate([att[o, src] for o in chunks], axis=0),
                    weights[src * width:(src + 1) * width, :],
                    preferred_element_type=F32,
                )
            result = total.astype(BF)
        for g, o in enumerate(chunks):
            part = result[g * rows:(g + 1) * rows]

            @pl.when(o == z)
            def _():
                br[quarter(d)] = part

            @pl.when(o != z)
            def _():
                stage[o, d] = part
                d_copy(o, d).start()

    def gathered(i):
        for k in range(line_half):
            for sd_of in (side, 1 - side):
                c_copy(order(i, jnp.logical_not(low)), hub + onward * (k + 1), sd_of).wait_recv()

    gap = 2
    steps = n_u + 1 + gap * (line_half - 2)

    def pass_step(t, _):
        for k in range(1, line_half):
            pass_on(t - gap * (k - 1), k)

        @pl.when(is_hub & (t == 2))
        def _():
            w_relay(SPLIT, 1)
            w_relay(2 * SPLIT, 0)

        i = t - (steps - line_half)

        @pl.when(is_hub & (i >= 0))
        def _():
            gathered(i)
            mix([i], wo_ref, 0)

        return 0

    with jax.named_scope("pass_loop"):
        @pl.when(is_hub)
        def _():
            wo_whole.wait()

        lax.fori_loop(0, steps, pass_step, 0)

    with jax.named_scope("hub"):
        @pl.when(is_hub)
        def _():
            with jax.named_scope("w_last"):
                for mask in sorted(masks, key=depth_of):
                    if mask % 2 == 0 and mask not in (SPLIT, 2 * SPLIT, *Z_MASKS):
                        for part in range(2):
                            w_relay(mask, part)
                drain(wx_ref.at[:, pl.ds(0, n_blk // 2 * slice_rows)], rw_core)

            for d in range(1, line_half):
                mix(range(line_half), wx_ref.at[d - 1], d)

            def near_mix(i, _):
                gathered(i)
                mix([i], wo_ref, 0)
                for d in range(1, line_half):
                    mix([i], wx_ref.at[d - 1], d)
                return 0

            lax.fori_loop(line_half, n_u, near_mix, 0)

    with jax.named_scope("final"):
        for src in range(n_u):
            @pl.when(jnp.logical_not(is_hub) | (low != (src < line_half)))
            def _():
                pltpu.make_async_remote_copy(
                    src_ref=br.at[src], dst_ref=br.at[src],
                    send_sem=rd.at[src], recv_sem=rd.at[src],
                    device_id={"ulysses": last - hub}, device_id_type=MESH,
                ).wait_recv()

            at = slice(src * width, (src + 1) * width)
            out_ref[:, at] = (
                tok_ref[:, at].astype(F32) + gate_ref[:, at] * br[src].astype(F32)
            ).astype(BF)

    def finish(s, _):
        for u in range(2):
            @pl.when((s <= z) & (z < last))
            def _():
                a_right(2 * s + u).wait_send()

            @pl.when((s >= z) & (z > 0))
            def _():
                a_left(2 * s + u).wait_send()

        @pl.when(jnp.where(low, s <= z, s >= z))
        def _():
            drain(att.at[:, s], sc.at[s])

        return 0

    with jax.named_scope("finish"):
        lax.fori_loop(0, n_u, finish, 0)

        drain(xatt, sx)
        drain(q_ref.at[pl.ds(0, share), 0], sq)
        drain(kv.at[:, pl.ds(0, share), pl.ds(1, n_blk - 1)], sb)

        @pl.when(is_hub)
        def _():
            drain(stage.at[pl.ds(0, n_u - 1)], sd)
            drain(wx_ref.at[:, pl.ds(0, (n_blk - len(Z_MASKS)) * slice_rows)], sw)

        @pl.when(jnp.logical_not(is_hub))
        def _():
            for i in range(len(Z_MASKS)):
                for part in range(2):
                    wz_copy(i, part, away - 1).wait_send()


def local(n_u, n_blk, tokens, mod_shift, mod_scale, mod_gate, qkv_weight, query_gain, key_gain, out_weight):
    rows, model = tokens.shape
    width = qkv_weight.shape[2]
    head = query_gain.shape[0]
    heads = width // head
    vmem = pl.BlockSpec(memory_space=pltpu.VMEM)
    hbm = pl.BlockSpec(memory_space=pltpu.HBM)
    dma = pltpu.SemaphoreType.DMA
    split = heads % 2 == 0 and n_blk % (4 * SPLIT) == 0 and n_u % 2 == 0 and n_u > 2
    buffers = [
        pltpu.VMEM(qkv_weight.shape, BF),
        pltpu.VMEM(out_weight.shape, BF),
        pltpu.VMEM((2 * n_u, rows // 2, model), BF),
    ]
    line_sems = [dma((4,)), dma((2 * n_u,)), dma((2 * n_u,)), dma((2 * n_u,))]
    block_sems = [dma((n_blk, 2, 2 * n_u)), dma((n_blk, 2, 2 * n_u))]
    keys = pltpu.VMEM((2, heads, n_blk, 2 * n_u, rows // 2, head), BF)
    attended = pltpu.VMEM((n_u, n_u, rows, width), BF)
    mixed = pltpu.VMEM((n_u, rows, width), BF)
    row = pltpu.VMEM((1, model), F32)
    early = hbm if split else vmem
    one = pltpu.SemaphoreType.DMA
    if split:
        body = split_kernel
        scratch = buffers + [
            pltpu.VMEM((heads, 2, 2 * n_u, rows // 2, head), BF), keys,
            pltpu.VMEM((n_u // 2 - 1, *out_weight.shape), BF),
            attended, pltpu.VMEM((n_u, rows, width // 2), BF),
            pltpu.VMEM((n_u, n_u // 2, rows, width), BF), mixed,
            pltpu.VMEM((rows, model), BF), row, row, row, dma((4,)),
            dma((2, 2)), dma((n_u // 2 - 1, 2, 2)), one, dma((n_blk // 2, 2)), one,
            dma((5,)),
        ] + line_sems[1:] + [
            one, dma((n_blk // 2 - 1, 2, n_u + 1)), one, one, one, one, dma((n_u,)),
            dma((n_u,)), dma((n_u, n_u, 2)), one, dma((n_u,)),
        ]
    else:
        body = kernel
        scratch = buffers + [
            pltpu.VMEM((heads, 2 * n_u, rows // 2, head), BF), keys,
            attended, mixed, mixed,
        ] + line_sems + block_sems + [
            dma((n_u, n_u)), dma((n_u, n_u)), dma((n_u, n_u)),
            dma((n_u,)), dma((n_u,)),
        ]
    return pl.pallas_call(
        functools.partial(body, n_u, n_blk),
        out_shape=pltpu.VMEM((rows, model), BF) if split else jax.ShapeDtypeStruct((rows, model), BF),
        in_specs=[early, early, early, early, hbm, vmem, vmem, hbm],
        out_specs=vmem,
        scratch_shapes=scratch,
        compiler_params=pltpu.CompilerParams(
            collective_id=0, has_side_effects=True, vmem_limit_bytes=63_000_000 if split else 66_000_000
        ),
    )(
        tokens, mod_shift[None], mod_scale[None], mod_gate[None],
        qkv_weight, query_gain[None], key_gain[None], out_weight,
    )


def solution(mesh):
    in_specs = (
        P(("blk", "ulysses"), None), P(), P(), P(),
        P(None, None, "ulysses"), P(), P(), P(None, "ulysses"),
    )
    out_specs = P(("blk", "ulysses"), None)
    body = functools.partial(local, mesh.shape["ulysses"], mesh.shape["blk"])
    return jax.shard_map(body, mesh=mesh, in_specs=in_specs, out_specs=out_specs, check_vma=False)
```
